256 devices in a mesh: gx: 8 (over z), gy: 4 (over y_lo, core), gz: 8 (over y_hi, x).
Axes of the slice: x: 4, y: 4 (y_hi: 2, y_lo: 2; y = y_hi * 2 + y_lo), z: 8, core: 2. Of those that a mesh axis runs over, the one named last changes fastest.
Arguments:
- incident: bfloat16 [8, 4, 8, 2, 1280, 128], P('gx', 'gy', 'gz'), may hold values from -6 to 6
- response: bfloat16 [8, 4, 8, 2, 1280, 1280], P('gx', 'gy', 'gz'), may hold values from -0.125 to 0.125
- radiation: bfloat16 [8, 4, 8, 2, 512, 1280], P('gx', 'gy', 'gz'), may hold values from -0.0078125 to 0.0078125
- face_index: int32 [8, 4, 8, 6, 192], P('gx', 'gy', 'gz'), may hold values from 0 to 1279, as said below
- linked: int32 [8, 4, 8, 6], P('gx', 'gy', 'gz'), may hold values 0 or 1
Outputs:
- far_field: float32 [2, 128, 512], P(None, ('gx', 'gy'), 'gz')
The draws below stay inside these ranges and needn't reach their ends.
Inputs may be any that keep to these rules, and one draw needn't show every extreme that they name: `face_index`: the 1152 entries of one subdomain are distinct.
All inputs are finite; a program needn't handle non-finite values. No bound on the sum of `linked` on one device may be relied on, other than what follows from the above.
Results may differ from the reference program's by a relative error of at most 0.004.
Values may be sent and summed in bfloat16 or wider, within the bound.
A program may use at most 64 MiB of HBM per device.

```python
import jax
import jax.numpy as jnp
from jax import lax

M = 1280
FACE = 192
ANG = 512
EXC = 128
ITERS = 2
N_GX = 8
N_GY = 4
N_GZ = 8


def draw_face_index(key, part):
    keys = jax.random.split(jax.random.fold_in(key, 17), N_GX * N_GY * N_GZ)
    picks = jax.vmap(lambda single: jax.random.permutation(single, M)[:6 * FACE])(keys)
    return picks.reshape(N_GX, N_GY, N_GZ, 6, FACE).astype(jnp.int32)


def with_ends(result, rng, low, high):
    longest = result.shape.index(max(result.shape))
    spots = []
    for shift in (0, 1):
        where = [jax.random.randint(jax.random.fold_in(rng, axis), (), 0, length) for axis, length in enumerate(result.shape)]
        where[longest] = (where[longest] + shift) % result.shape[longest]
        spots.append(tuple(where))
    return result.at[spots[0]].set(low).at[spots[1]].set(high)


def level_of(key, dims, cuts, least, top_value):
    loudness = 1.0
    for dim, shards_of in cuts:
        heights = jax.random.uniform(jax.random.fold_in(jax.random.fold_in(key, 6), dim), (shards_of,), jnp.float32, least / len(cuts), top_value / len(cuts))
        loudness = loudness * jnp.repeat(jnp.exp(heights), dims[dim] // shards_of).reshape((-1,) + (1,) * (len(dims) - 1 - dim))
    return loudness


def gaussian(stream_key, dims, scale, most, shards=(), kind=jnp.bfloat16):
    array = scale * jax.random.normal(stream_key, dims, jnp.float32)
    if shards:
        array = array * level_of(stream_key, dims, shards, -0.22, 0.18)
    return jnp.clip(array, -most, most).astype(kind)


def setup_inputs(seed: int = 0) -> dict:
    arg_keys = jax.random.split(jax.random.key(seed), 6)
    incident = gaussian(arg_keys[0], (N_GX, N_GY, N_GZ, 2, M, EXC), 1.0, 6.0, ((0, 8), (1, 4), (2, 8)))
    response = gaussian(arg_keys[1], (N_GX, N_GY, N_GZ, 2, M, M), (2 * M) ** -0.5, 0.125, ((0, 8), (1, 4), (2, 8)))
    radiation = gaussian(arg_keys[2], (N_GX, N_GY, N_GZ, 2, ANG, M), (2 * M * N_GX * N_GY * N_GZ) ** -0.5, 0.0078125, ((0, 8), (1, 4), (2, 8)))
    face_index = draw_face_index(jax.random.fold_in(arg_keys[5], 71), 0)
    linked = with_ends((jax.random.randint(arg_keys[4], (N_GX, N_GY, N_GZ, 6), 0, 4) < 3).astype(jnp.int32), jax.random.fold_in(arg_keys[4], 1), 0, 1)
    return dict(incident=incident, response=response, radiation=radiation, face_index=face_index, linked=linked)


def complex_dot(left_side, right_side):
    real_part = jnp.dot(left_side[0], right_side[0], preferred_element_type=jnp.float32) - jnp.dot(left_side[1], right_side[1], preferred_element_type=jnp.float32)
    imag_part = jnp.dot(left_side[0], right_side[1], preferred_element_type=jnp.float32) + jnp.dot(left_side[1], right_side[0], preferred_element_type=jnp.float32)
    return jnp.stack([real_part, imag_part])


def from_lower(values, dim):
    blank = jnp.zeros_like(lax.slice_in_dim(values, 0, 1, axis=dim))
    return jnp.concatenate([blank, lax.slice_in_dim(values, 0, values.shape[dim] - 1, axis=dim)], dim)


def from_upper(values, dim):
    blank = jnp.zeros_like(lax.slice_in_dim(values, 0, 1, axis=dim))
    return jnp.concatenate([lax.slice_in_dim(values, 1, values.shape[dim], axis=dim), blank], dim)


def place_rows(slots, values):
    blank = jnp.zeros((2, M, values.shape[-1]), values.dtype)
    return blank.at[:, slots].set(values.reshape(2, 6 * FACE, values.shape[-1]))


def reference(incident, response, radiation, face_index, linked):
    count = N_GX * N_GY * N_GZ
    flat_incident = incident.reshape(count, 2, M, EXC)
    flat_response = response.reshape(count, 2, M, M)
    flat_radiation = radiation.reshape(count, 2, ANG, M)
    flat_slots = face_index.reshape(count, 6 * FACE).astype(jnp.int32)
    flat_linked = linked.reshape(count, 6)
    traces = jnp.zeros((count, 2, M, EXC), incident.dtype)
    for sweep in range(ITERS):
        summed = (traces.astype(jnp.float32) + flat_incident.astype(jnp.float32)).astype(jnp.bfloat16)
        outgoing = lax.map(lambda pair: complex_dot(pair[0], pair[1]).astype(jnp.bfloat16), (flat_response, summed))
        faces = jax.vmap(lambda rows, slots: rows[:, slots, :])(outgoing, flat_slots)
        faces = faces.reshape(N_GX, N_GY, N_GZ, 2, 6, FACE, EXC)
        arrived = []
        for axis_pos in range(3):
            arrived.append(from_lower(faces[:, :, :, :, 2 * axis_pos + 1], axis_pos))
            arrived.append(from_upper(faces[:, :, :, :, 2 * axis_pos], axis_pos))
        incoming = jnp.stack(arrived, 4).reshape(count, 2, 6, FACE, EXC)
        incoming = incoming * flat_linked[:, None, :, None, None].astype(incoming.dtype)
        traces = jax.vmap(place_rows)(flat_slots, incoming)
    currents = (traces.astype(jnp.float32) + flat_incident.astype(jnp.float32)).astype(jnp.bfloat16)

    def accumulate(total, pair):
        return total + complex_dot(pair[0], pair[1]), None

    total, unused = lax.scan(accumulate, jnp.zeros((2, ANG, EXC), jnp.float32), (flat_radiation, currents))
    return jnp.transpose(total, (0, 2, 1))
```

```python
import functools

import jax
import jax.numpy as jnp
from jax import lax
from jax.experimental import pallas as pl
from jax.experimental.pallas import tpu as pltpu
from jax.sharding import PartitionSpec as P

M = 1280
FACE = 192
ANG = 512
EXC = 128
PADDED = 256
CHUNKS = 5
ROWS = M // CHUNKS
PARTS = 4
PART_ROWS = ANG // PARTS
BLOCK = 64
MESH = pl.DeviceIdType.MESH
PICK_ORDER = (4, 5, 0, 1, 3, 2)
BF16, F32 = jnp.bfloat16, jnp.float32


def plane_order():
    steps = [(a, b, c) for a in range(2) for b in range(4) for c in range(2) if (a, b, c) != (0, 0, 0)]
    return sorted(steps, key=lambda s: -((2 if s[1] == 2 else s[1] % 2) + (1 if s[2] else 2 * s[0])))


def kernel(
    incident, response, radiation, face_index, linked, out_ref,
    inc, resp, rad, slots_raw, slots, link, select, place, weights, outgoing, sent, arrived, total,
    keep, half_out, half_in, plane_out, plane_in, line_out, line_in,
    load_sem, resp_sem, face_send, face_recv, half_send, half_recv, plane_send, plane_recv, line_send, line_recv,
):
    gx, gy, gz = lax.axis_index("gx"), lax.axis_index("gy"), lax.axis_index("gz")
    core, y_lo = gy % 2, gy // 2
    x, y_hi = gz % 4, gz // 4
    me_plane = gz * 2 + y_lo
    coords = (gx, gy, gz)
    sizes = (8, 4, 8)

    loads = [
        pltpu.make_async_copy(incident, inc, load_sem.at[0]),
        pltpu.make_async_copy(face_index, slots_raw, load_sem.at[1]),
        pltpu.make_async_copy(linked, link, load_sem.at[2]),
    ]
    for load in loads:
        load.start()
    resp_loads = []
    for c in range(CHUNKS):
        rows = pl.ds(c * ROWS, ROWS)
        pair = [
            pltpu.make_async_copy(response.at[p, rows], resp.at[rows, pl.ds(p * M, M)], resp_sem.at[c, p])
            for p in range(2)
        ]
        for load in pair:
            load.start()
        resp_loads.append(pair)
    rad_loads = [
        pltpu.make_async_copy(radiation.at[p], rad.at[:, pl.ds(p * M, M)], load_sem.at[3 + p]) for p in range(2)
    ]
    for load in rad_loads:
        load.start()

    arrived[...] = jnp.zeros_like(arrived)
    plane_in[...] = jnp.zeros_like(plane_in)
    line_in[...] = jnp.zeros_like(line_in)

    barrier = pltpu.get_barrier_semaphore()

    def greet(device):
        pl.semaphore_signal(barrier, inc=1, device_id=device, device_id_type=MESH)

    def plane_peer(step):
        dyh, dx, dyl = step
        peer_gz = ((y_hi + dyh) % 2) * 4 + (x + dx) % 4
        peer_lo = (y_lo + dyl) % 2
        return peer_gz * 2 + peer_lo, (gx, peer_lo * 2 + core, peer_gz)

    order = plane_order()
    partner = (gx, gy + 1 - 2 * core, gz)
    cross = (gx, 3 - gy, gz)
    middle = (gy + 1) // 2 == 1
    for step in order:
        greet(plane_peer(step)[1])
    for d in range(1, 8):
        greet(((gx + d) % 8, gy, gz))
    greet(partner)

    @pl.when(middle)
    def _():
        greet(cross)

    slots[...] = jnp.full(slots.shape, -1, jnp.int32)
    loads[1].wait()
    slots[0:6, 0:FACE] = slots_raw[...]
    columns = lax.broadcasted_iota(jnp.int32, (128, 128), 1).astype(F32)
    for f in PICK_ORDER:
        row = slots[f : f + 1, :].astype(F32)
        for half, count in ((0, 128), (1, 64)):
            wide = jnp.broadcast_to(row[:, half * 128 : (half + 1) * 128], (128, 128))
            tall = jnp.transpose(wide)[:count]
            for c in range(M // 128):
                hit = tall - float(c * 128) == columns[:count]
                select[f, half * 128 : half * 128 + count, c * 128 : (c + 1) * 128] = jnp.where(hit, 1.0, 0.0).astype(BF16)

    def set_weights(rows, real, imag):
        low = pl.ds(rows.start, rows.size)
        high = pl.ds(M + rows.start, rows.size)
        weights[low, 0:EXC] = real
        weights[low, EXC : 2 * EXC] = imag
        weights[high, 0:EXC] = -imag
        weights[high, EXC : 2 * EXC] = real

    loads[0].wait()
    for c in range(CHUNKS):
        rows = pl.ds(c * ROWS, ROWS)
        set_weights(rows, inc[0, rows], inc[1, rows])

    def respond(first):
        for c in range(CHUNKS):
            rows = pl.ds(c * ROWS, ROWS)
            if first:
                for load in resp_loads[c]:
                    load.wait()
            outgoing[rows] = jnp.dot(resp[rows], weights[...], preferred_element_type=F32).astype(BF16)

    def neighbour(f):
        axis, up = f // 2, f % 2
        place_of = coords[axis]
        there = place_of < sizes[axis] - 1 if up else place_of > 0
        to = tuple(v + (1 if up else -1) if a == axis else v for a, v in enumerate(coords))
        return there, to

    def face_copy(it, f):
        there, to = neighbour(f)
        landing = f + 1 - 2 * (f % 2)
        return there, pltpu.make_async_remote_copy(
            src_ref=sent.at[it, f],
            dst_ref=arrived.at[it, pl.ds(landing * PADDED, FACE)],
            send_sem=face_send.at[it, f],
            recv_sem=face_recv.at[it, landing],
            device_id=to,
            device_id_type=MESH,
        )

    def send_faces(it):
        for f in PICK_ORDER:
            sent[it, f] = jnp.dot(select[f], outgoing[...], preferred_element_type=F32).astype(BF16)
            there, copy = face_copy(it, f)

            @pl.when(there)
            def _():
                copy.start()

    def take_faces(it, faces):
        for f in faces:
            there, _ = neighbour(f)

            @pl.when(there)
            def _():
                pltpu.make_async_remote_copy(
                    src_ref=sent.at[it, f],
                    dst_ref=arrived.at[it, pl.ds(f * PADDED, FACE)],
                    send_sem=face_send.at[it, f],
                    recv_sem=face_recv.at[it, f],
                    device_id=neighbour(f)[1],
                    device_id_type=MESH,
                ).wait_recv()

    def add_traces(it):
        take_faces(it, (0, 1, 2, 3))
        near = 4 * PADDED
        for c in range(CHUNKS):
            rows = pl.ds(c * ROWS, ROWS)
            total[rows] = jnp.dot(place[rows, 0:near], arrived[it, 0:near], preferred_element_type=F32)
        take_faces(it, (4, 5))
        for c in range(CHUNKS):
            rows = pl.ds(c * ROWS, ROWS)
            trace = total[rows] + jnp.dot(
                place[rows, near : 6 * PADDED], arrived[it, near : 6 * PADDED], preferred_element_type=F32
            )
            real = (trace[:, 0:EXC] + inc[0, rows].astype(F32)).astype(BF16)
            imag = (trace[:, EXC : 2 * EXC] + inc[1, rows].astype(F32)).astype(BF16)
            set_weights(rows, real, imag)

    respond(True)
    pl.semaphore_wait(barrier, 15 + 7 + 1 + jnp.where(middle, 1, 0))
    send_faces(0)

    loads[2].wait()
    for f in range(6):
        row = jnp.where(link[0, f] > 0, slots[f : f + 1, :], -1)
        for c in range(CHUNKS):
            spots = lax.broadcasted_iota(jnp.int32, (ROWS, PADDED), 0) + c * ROWS
            place[c * ROWS : (c + 1) * ROWS, f * PADDED : (f + 1) * PADDED] = jnp.where(spots == row, 1.0, 0.0).astype(BF16)

    add_traces(0)
    respond(False)
    send_faces(1)
    add_traces(1)

    lanes = lax.broadcasted_iota(jnp.int32, (PART_ROWS, EXC), 1)
    odd_core = (lanes // 4) % 2
    for load in rad_loads:
        load.wait()
    half_copies = []
    for q in range(PARTS):
        rows = pl.ds(q * PART_ROWS, PART_ROWS)
        field = jnp.dot(rad[rows], weights[...], preferred_element_type=F32)
        real, imag = field[:, 0:EXC], field[:, EXC : 2 * EXC]
        zero = jnp.where(odd_core == 0, real, pltpu.roll(imag, 4, 1))
        one = jnp.where(odd_core == 0, pltpu.roll(real, EXC - 4, 1), imag)
        keep[rows] = jnp.where(core == 0, zero, one)
        half_out[rows] = jnp.where(core == 0, one, zero)
        copy = pltpu.make_async_remote_copy(
            src_ref=half_out.at[rows],
            dst_ref=half_in.at[rows],
            send_sem=half_send.at[q],
            recv_sem=half_recv.at[q],
            device_id=partner,
            device_id_type=MESH,
        )
        copy.start()
        half_copies.append(copy)

    small = lax.broadcasted_iota(jnp.int32, (BLOCK // 2, EXC), 1)
    odd_lo = (small // 8) % 2
    for q in range(PARTS):
        half_copies[q].wait_recv()
        for b in range(PART_ROWS // BLOCK):
            start = q * PART_ROWS + b * BLOCK
            first = pl.ds(start, BLOCK // 2)
            second = pl.ds(start + BLOCK // 2, BLOCK // 2)
            top = keep[first] + half_in[first]
            low = keep[second] + half_in[second]
            slot = (q * (PART_ROWS // BLOCK) + b) * 2
            plane_out[slot] = jnp.where(odd_lo == 0, top, pltpu.roll(low, 8, 1)).astype(BF16)
            plane_out[slot + 1] = jnp.where(odd_lo == 0, pltpu.roll(top, EXC - 8, 1), low).astype(BF16)

    plane_copies = []
    for n, step in enumerate(order):
        peer, device = plane_peer(step)
        copy = pltpu.make_async_remote_copy(
            src_ref=plane_out.at[peer],
            dst_ref=plane_in.at[me_plane],
            send_sem=plane_send.at[n],
            recv_sem=plane_recv.at[me_plane],
            device_id=device,
            device_id_type=MESH,
        )
        copy.start()
        plane_copies.append(copy)
    for s in range(16):

        @pl.when(s != me_plane)
        def _():
            pltpu.make_async_remote_copy(
                src_ref=plane_out.at[s],
                dst_ref=plane_in.at[s],
                send_sem=plane_send.at[0],
                recv_sem=plane_recv.at[s],
                device_id=partner,
                device_id_type=MESH,
            ).wait_recv()

    piece = plane_out[me_plane].astype(F32)
    for s in range(16):
        piece = piece + plane_in[s].astype(F32)
    tall = jnp.concatenate([piece, pltpu.roll(piece, EXC - 8, 1)], axis=0)
    turned = jnp.transpose(jnp.concatenate([tall, tall], axis=0))
    for d in range(8):
        line_out[d] = turned[d * 16 : d * 16 + 8]
    line_copies = []
    for d in (4, 3, 5, 2, 6, 1, 7):
        peer = (gx + d) % 8
        copy = pltpu.make_async_remote_copy(
            src_ref=line_out.at[peer],
            dst_ref=line_in.at[gx],
            send_sem=line_send.at[d],
            recv_sem=line_recv.at[gx],
            device_id=(peer, gy, gz),
            device_id_type=MESH,
        )
        copy.start()
        line_copies.append(copy)
    for s in range(8):

        @pl.when(s != gx)
        def _():
            pltpu.make_async_remote_copy(
                src_ref=line_out.at[s],
                dst_ref=line_in.at[s],
                send_sem=line_send.at[0],
                recv_sem=line_recv.at[s],
                device_id=partner,
                device_id_type=MESH,
            ).wait_recv()

    result = line_out[gx]
    for s in range(8):
        result = result + line_in[s]
    out_ref[0] = result[0:4, 0:BLOCK]
    out_ref[1] = result[4:8, 0:BLOCK]

    for it in range(2):
        for f in range(6):
            there, copy = face_copy(it, f)

            @pl.when(there)
            def _():
                copy.wait_send()

    for copy in half_copies + plane_copies + line_copies:
        copy.wait_send()


def shards(incident, response, radiation, face_index, linked):
    anywhere = pl.BlockSpec(memory_space=pl.ANY)
    dma = pltpu.SemaphoreType.DMA
    return pl.pallas_call(
        kernel,
        out_shape=jax.ShapeDtypeStruct((2, 4, BLOCK), F32),
        in_specs=[anywhere] * 5,
        out_specs=pl.BlockSpec(memory_space=pltpu.VMEM),
        scratch_shapes=[
            pltpu.VMEM((2, M, EXC), BF16),
            pltpu.VMEM((M, 2 * M), BF16),
            pltpu.VMEM((ANG, 2 * M), BF16),
            pltpu.VMEM((6, FACE), jnp.int32),
            pltpu.VMEM((8, PADDED), jnp.int32),
            pltpu.SMEM((1, 6), jnp.int32),
            pltpu.VMEM((6, FACE, M), BF16),
            pltpu.VMEM((M, 6 * PADDED), BF16),
            pltpu.VMEM((2 * M, 2 * EXC), BF16),
            pltpu.VMEM((M, 2 * EXC), BF16),
            pltpu.VMEM((2, 6, FACE, 2 * EXC), BF16),
            pltpu.VMEM((2, 6 * PADDED, 2 * EXC), BF16),
            pltpu.VMEM((M, 2 * EXC), F32),
            pltpu.VMEM((ANG, EXC), F32),
            pltpu.VMEM((ANG, EXC), F32),
            pltpu.VMEM((ANG, EXC), F32),
            pltpu.VMEM((16, BLOCK // 2, EXC), BF16),
            pltpu.VMEM((16, BLOCK // 2, EXC), BF16),
            pltpu.VMEM((8, 8, EXC), F32),
            pltpu.VMEM((8, 8, EXC), F32),
            dma((5,)),
            dma((CHUNKS, 2)),
            dma((2, 6)),
            dma((2, 6)),
            dma((PARTS,)),
            dma((PARTS,)),
            dma((16,)),
            dma((16,)),
            dma((8,)),
            dma((8,)),
        ],
        compiler_params=pltpu.CompilerParams(
            collective_id=0, has_side_effects=True, vmem_limit_bytes=60 * 1024 * 1024
        ),
        cost_estimate=pl.CostEstimate(flops=8_000_000_000, bytes_accessed=10_000_000, transcendentals=0),
        name="schwarz",
    )(
        incident.reshape(2, M, EXC),
        response.reshape(2, M, M),
        radiation.reshape(2, ANG, M),
        face_index.reshape(6, FACE),
        linked.reshape(1, 6),
    )


def solution(mesh):
    return jax.shard_map(
        shards,
        mesh=mesh,
        in_specs=(
            P("gx", "gy", "gz", None, None, None),
            P("gx", "gy", "gz", None, None, None),
            P("gx", "gy", "gz", None, None, None),
            P("gx", "gy", "gz", None, None),
            P("gx", "gy", "gz", None),
        ),
        out_specs=P(None, ("gx", "gy"), "gz"),
        check_vma=False,
    )
```

```python
import functools

import jax
import jax.numpy as jnp
from jax import lax
from jax.experimental import pallas as pl
from jax.experimental.pallas import tpu as pltpu
from jax.sharding import PartitionSpec as P

M = 1280
FACE = 192
ANG = 512
EXC = 128
PADDED = 256
CHUNKS = 5
ROWS = M // CHUNKS
PARTS = 4
PART_ROWS = ANG // PARTS
BLOCK = 64
MESH = pl.DeviceIdType.MESH
PICK_ORDER = (4, 0, 1, 2, 3, 5)
TAKE_ORDER = (2, 0, 1)
BF16, F32 = jnp.bfloat16, jnp.float32


def plane_order():
    steps = [(a, b, c) for a in range(2) for b in range(4) for c in range(2) if (a, b, c) != (0, 0, 0)]
    return sorted(steps, key=lambda s: -((2 if s[1] == 2 else s[1] % 2) + (1 if s[2] else 2 * s[0])))


def kernel(
    incident, response, radiation, face_index, linked, out_ref,
    inc, resp, rad, slots_raw, slots, link, select, place, weights, outgoing, sent, near_in, far_in, total, columns, field,
    keep, half_out, half_in, plane_out, plane_in, line_out, line_in,
    load_sem, resp_sem, face_send, face_recv, half_send, half_recv, plane_send, plane_recv, line_send, line_recv,
):
    loads = [
        pltpu.make_async_copy(face_index, slots_raw, load_sem.at[0]),
        pltpu.make_async_copy(incident, inc, load_sem.at[1]),
        pltpu.make_async_copy(linked, link, load_sem.at[2]),
    ]
    for load in loads:
        load.start()
    resp_loads = []
    for c in range(CHUNKS):
        rows = pl.ds(c * ROWS, ROWS)
        pair = [
            pltpu.make_async_copy(response.at[p, rows], resp.at[rows, pl.ds(p * M, M)], resp_sem.at[c, p])
            for p in range(2)
        ]
        for load in pair:
            load.start()
        resp_loads.append(pair)
    rad_loads = [
        pltpu.make_async_copy(radiation.at[p], rad.at[:, pl.ds(p * M, M)], load_sem.at[3 + p]) for p in range(2)
    ]

    gx, gy, gz = lax.axis_index("gx"), lax.axis_index("gy"), lax.axis_index("gz")
    core, y_lo = gy % 2, gy // 2
    x, y_hi = gz % 4, gz // 4
    me_plane = gz * 2 + y_lo

    near_in[...] = jnp.zeros_like(near_in)
    for g in range(3):
        far_in[g, 0 : 2 * PADDED] = jnp.zeros((2 * PADDED, 2 * EXC), BF16)
    plane_in[...] = jnp.zeros_like(plane_in)
    line_in[...] = jnp.zeros_like(line_in)

    barrier = pltpu.get_barrier_semaphore()

    def greet(device):
        pl.semaphore_signal(barrier, inc=1, device_id=device, device_id_type=MESH)

    def plane_peer(step):
        dyh, dx, dyl = step
        peer_gz = ((y_hi + dyh) % 2) * 4 + (x + dx) % 4
        peer_lo = (y_lo + dyl) % 2
        return peer_gz * 2 + peer_lo, (gx, peer_lo * 2 + core, peer_gz)

    order = plane_order()
    partner = (gx, gy + 1 - 2 * core, gz)
    cross = (gx, 3 - gy, gz)
    middle = (gy + 1) // 2 == 1
    for step in order:
        greet(plane_peer(step)[1])
    for d in range(1, 8):
        greet(((gx + d) % 8, gy, gz))
    greet(partner)

    @pl.when(middle)
    def _():
        greet(cross)

    ahead, across = core, 1 - core
    face_of = (4 * ahead, 4 * ahead + 1, 4 * across, 4 * across + 1, 2 + core, 3 - core)
    place_a, place_b = gx * across + gz * ahead, gx * ahead + gz * across
    there = (place_a > 0, place_a < 7, place_b > 0, place_b < 7, middle, None)
    target = (
        (gx - across, gy, gz - ahead),
        (gx + across, gy, gz + ahead),
        (gx - ahead, gy, gz - across),
        (gx + ahead, gy, gz + across),
        cross,
        partner,
    )
    landing = (1, 0, 3, 2, 4, 5)

    def guarded(role, action):
        if there[role] is None:
            action()
        else:
            pl.when(there[role])(action)

    slots[...] = jnp.full(slots.shape, -1, jnp.int32)
    loads[0].wait()
    for f in range(6):
        slots[f : f + 1, 0:FACE] = slots_raw[f]
    lanes128 = lax.broadcasted_iota(jnp.int32, (128, 128), 1).astype(F32)
    for r in PICK_ORDER:
        row = slots[pl.ds(face_of[r], 1), :].astype(F32)
        for half, count in ((0, 128), (1, 64)):
            wide = jnp.broadcast_to(row[:, half * 128 : (half + 1) * 128], (128, 128))
            tall = jnp.transpose(wide)[:count]
            for c in range(M // 128):
                hit = tall - float(c * 128) == lanes128[:count]
                select[r, half * 128 : half * 128 + count, c * 128 : (c + 1) * 128] = jnp.where(hit, 1.0, 0.0).astype(BF16)

    def set_weights(rows, real, imag):
        low = pl.ds(rows.start, rows.size)
        high = pl.ds(M + rows.start, rows.size)
        weights[low, 0:EXC] = real
        weights[low, EXC : 2 * EXC] = imag
        weights[high, 0:EXC] = -imag
        weights[high, EXC : 2 * EXC] = real

    loads[1].wait()
    for c in range(CHUNKS):
        rows = pl.ds(c * ROWS, ROWS)
        set_weights(rows, inc[0, rows], inc[1, rows])

    def respond(first):
        for c in range(CHUNKS):
            rows = pl.ds(c * ROWS, ROWS)
            if first:
                for load in resp_loads[c]:
                    load.wait()
                if c == CHUNKS - 2:
                    for load in rad_loads:
                        load.start()
            outgoing[rows] = jnp.dot(resp[rows], weights[...], preferred_element_type=F32).astype(BF16)

    def face_copy(it, role, to=None):
        spot = landing[role] if to is None else to
        if it == 0:
            dst = near_in.at[pl.ds(spot * PADDED, FACE)]
        else:
            dst = far_in.at[spot // 2, pl.ds((spot % 2) * PADDED, FACE)]
        return pltpu.make_async_remote_copy(
            src_ref=sent.at[it, role],
            dst_ref=dst,
            send_sem=face_send.at[it, role],
            recv_sem=face_recv.at[it, spot],
            device_id=target[role],
            device_id_type=MESH,
        )

    def send_faces(it):
        for r in PICK_ORDER:
            sent[it, r] = jnp.dot(select[r], outgoing[...], preferred_element_type=F32).astype(BF16)
            guarded(r, face_copy(it, r).start)

    def take_faces(it, roles):
        for r in roles:
            guarded(r, face_copy(it, r, r).wait_recv)

    def add_traces():
        for n, g in enumerate(TAKE_ORDER):
            take_faces(0, (2 * g, 2 * g + 1))
            span = slice(2 * g * PADDED, (2 * g + 2) * PADDED)
            for c in range(CHUNKS):
                rows = pl.ds(c * ROWS, ROWS)
                trace = jnp.dot(place[rows, span], near_in[span], preferred_element_type=F32)
                if n > 0:
                    trace = trace + total[rows]
                if n < 2:
                    total[rows] = trace
                else:
                    real = (trace[:, 0:EXC] + inc[0, rows].astype(F32)).astype(BF16)
                    imag = (trace[:, EXC : 2 * EXC] + inc[1, rows].astype(F32)).astype(BF16)
                    set_weights(rows, real, imag)

    def gather_columns(g, p):
        picked = jnp.dot(
            rad[:, p * M : (p + 1) * M], place[:, 2 * g * PADDED : (2 * g + 2) * PADDED], preferred_element_type=F32
        )
        columns[g, :, 2 * p * PADDED : (2 * p + 2) * PADDED] = picked.astype(BF16)

    respond(True)
    pl.semaphore_wait(barrier, 15 + 7 + 1 + jnp.where(middle, 1, 0))
    send_faces(0)

    for load in rad_loads:
        load.wait()
    field[...] = jnp.dot(rad[...], weights[...], preferred_element_type=F32)
    loads[2].wait()
    for r in range(6):
        row = jnp.where(link[0, face_of[r]] > 0, slots[pl.ds(face_of[r], 1), :], -1)
        for c in range(CHUNKS):
            spots = lax.broadcasted_iota(jnp.int32, (ROWS, PADDED), 0) + c * ROWS
            place[c * ROWS : (c + 1) * ROWS, r * PADDED : (r + 1) * PADDED] = jnp.where(spots == row, 1.0, 0.0).astype(BF16)
    gather_columns(TAKE_ORDER[0], 0)
    gather_columns(TAKE_ORDER[0], 1)

    add_traces()
    respond(False)
    send_faces(1)
    for g in TAKE_ORDER[1:]:
        gather_columns(g, 0)
        gather_columns(g, 1)

    lanes = lax.broadcasted_iota(jnp.int32, (PART_ROWS, EXC), 1)
    odd_core = (lanes // 4) % 2
    half_copies = []
    for n, g in enumerate(TAKE_ORDER):
        take_faces(1, (2 * g, 2 * g + 1))
        low, high = slice(0, 2 * PADDED), slice(2 * PADDED, 4 * PADDED)
        far_in[g, high, 0:EXC] = -far_in[g, low, EXC : 2 * EXC]
        far_in[g, high, EXC : 2 * EXC] = far_in[g, low, 0:EXC]
        for q in range(PARTS):
            rows = pl.ds(q * PART_ROWS, PART_ROWS)
            value = field[rows] + jnp.dot(columns[g, rows], far_in[g], preferred_element_type=F32)
            if n < 2:
                field[rows] = value
                continue
            real, imag = value[:, 0:EXC], value[:, EXC : 2 * EXC]
            zero = jnp.where(odd_core == 0, real, pltpu.roll(imag, 4, 1))
            one = jnp.where(odd_core == 0, pltpu.roll(real, EXC - 4, 1), imag)
            keep[rows] = jnp.where(core == 0, zero, one)
            half_out[rows] = jnp.where(core == 0, one, zero)
            copy = pltpu.make_async_remote_copy(
                src_ref=half_out.at[rows],
                dst_ref=half_in.at[rows],
                send_sem=half_send.at[q],
                recv_sem=half_recv.at[q],
                device_id=partner,
                device_id_type=MESH,
            )
            copy.start()
            half_copies.append(copy)

    small = lax.broadcasted_iota(jnp.int32, (BLOCK // 2, EXC), 1)
    odd_lo = (small // 8) % 2
    for q in range(PARTS):
        half_copies[q].wait_recv()
        for b in range(PART_ROWS // BLOCK):
            start = q * PART_ROWS + b * BLOCK
            first = pl.ds(start, BLOCK // 2)
            second = pl.ds(start + BLOCK // 2, BLOCK // 2)
            top = keep[first] + half_in[first]
            low = keep[second] + half_in[second]
            slot = (q * (PART_ROWS // BLOCK) + b) * 2
            plane_out[slot] = jnp.where(odd_lo == 0, top, pltpu.roll(low, 8, 1)).astype(BF16)
            plane_out[slot + 1] = jnp.where(odd_lo == 0, pltpu.roll(top, EXC - 8, 1), low).astype(BF16)

    plane_copies = []
    for n, step in enumerate(order):
        peer, device = plane_peer(step)
        copy = pltpu.make_async_remote_copy(
            src_ref=plane_out.at[peer],
            dst_ref=plane_in.at[me_plane],
            send_sem=plane_send.at[n],
            recv_sem=plane_recv.at[me_plane],
            device_id=device,
            device_id_type=MESH,
        )
        copy.start()
        plane_copies.append(copy)
    for s in range(16):

        @pl.when(s != me_plane)
        def _():
            pltpu.make_async_remote_copy(
                src_ref=plane_out.at[s],
                dst_ref=plane_in.at[s],
                send_sem=plane_send.at[0],
                recv_sem=plane_recv.at[s],
                device_id=partner,
                device_id_type=MESH,
            ).wait_recv()

    piece = plane_out[me_plane].astype(F32)
    for s in range(16):
        piece = piece + plane_in[s].astype(F32)
    tall = jnp.concatenate([piece, pltpu.roll(piece, EXC - 8, 1)], axis=0)
    turned = jnp.transpose(jnp.concatenate([tall, tall], axis=0))
    for d in range(8):
        line_out[d] = turned[d * 16 : d * 16 + 8]
    line_copies = []
    for d in (4, 3, 5, 2, 6, 1, 7):
        peer = (gx + d) % 8
        copy = pltpu.make_async_remote_copy(
            src_ref=line_out.at[peer],
            dst_ref=line_in.at[gx],
            send_sem=line_send.at[d],
            recv_sem=line_recv.at[gx],
            device_id=(peer, gy, gz),
            device_id_type=MESH,
        )
        copy.start()
        line_copies.append(copy)

    for it in range(2):
        for r in range(6):
            guarded(r, face_copy(it, r).wait_send)
    for copy in half_copies + plane_copies:
        copy.wait_send()

    for s in range(8):

        @pl.when(s != gx)
        def _():
            pltpu.make_async_remote_copy(
                src_ref=line_out.at[s],
                dst_ref=line_in.at[s],
                send_sem=line_send.at[0],
                recv_sem=line_recv.at[s],
                device_id=partner,
                device_id_type=MESH,
            ).wait_recv()

    result = line_out[gx]
    for s in range(8):
        result = result + line_in[s]
    out_ref[0] = result[0:4, 0:BLOCK]
    out_ref[1] = result[4:8, 0:BLOCK]
    for copy in line_copies:
        copy.wait_send()


def shards(incident, response, radiation, face_index, linked):
    anywhere = pl.BlockSpec(memory_space=pl.ANY)
    dma = pltpu.SemaphoreType.DMA
    return pl.pallas_call(
        kernel,
        out_shape=pltpu.VMEM((2, 4, BLOCK), F32),
        in_specs=[anywhere] * 5,
        out_specs=pl.BlockSpec(memory_space=pltpu.VMEM),
        scratch_shapes=[
            pltpu.VMEM((2, M, EXC), BF16),
            pltpu.VMEM((M, 2 * M), BF16),
            pltpu.VMEM((ANG, 2 * M), BF16),
            pltpu.VMEM((6, 1, FACE), jnp.int32),
            pltpu.VMEM((8, PADDED), jnp.int32),
            pltpu.SMEM((1, 6), jnp.int32),
            pltpu.VMEM((6, FACE, M), BF16),
            pltpu.VMEM((M, 6 * PADDED), BF16),
            pltpu.VMEM((2 * M, 2 * EXC), BF16),
            pltpu.VMEM((M, 2 * EXC), BF16),
            pltpu.VMEM((2, 6, FACE, 2 * EXC), BF16),
            pltpu.VMEM((6 * PADDED, 2 * EXC), BF16),
            pltpu.VMEM((3, 4 * PADDED, 2 * EXC), BF16),
            pltpu.VMEM((M, 2 * EXC), F32),
            pltpu.VMEM((3, ANG, 4 * PADDED), BF16),
            pltpu.VMEM((ANG, 2 * EXC), F32),
            pltpu.VMEM((ANG, EXC), F32),
            pltpu.VMEM((ANG, EXC), F32),
            pltpu.VMEM((ANG, EXC), F32),
            pltpu.VMEM((16, BLOCK // 2, EXC), BF16),
            pltpu.VMEM((16, BLOCK // 2, EXC), BF16),
            pltpu.VMEM((8, 8, EXC), F32),
            pltpu.VMEM((8, 8, EXC), F32),
            dma((5,)),
            dma((CHUNKS, 2)),
            dma((2, 6)),
            dma((2, 6)),
            dma((PARTS,)),
            dma((PARTS,)),
            dma((16,)),
            dma((16,)),
            dma((8,)),
            dma((8,)),
        ],
        compiler_params=pltpu.CompilerParams(
            collective_id=0, has_side_effects=True, vmem_limit_bytes=60 * 1024 * 1024
        ),
        cost_estimate=pl.CostEstimate(flops=8_000_000_000, bytes_accessed=10_000_000, transcendentals=0),
        name="schwarz",
    )(
        incident.reshape(2, M, EXC),
        response.reshape(2, M, M),
        radiation.reshape(2, ANG, M),
        face_index.reshape(6, 1, FACE),
        linked.reshape(1, 6),
    )


def solution(mesh):
    return jax.shard_map(
        shards,
        mesh=mesh,
        in_specs=(
            P("gx", "gy", "gz", None, None, None),
            P("gx", "gy", "gz", None, None, None),
            P("gx", "gy", "gz", None, None, None),
            P("gx", "gy", "gz", None, None),
            P("gx", "gy", "gz", None),
        ),
        out_specs=P(None, ("gx", "gy"), "gz"),
        check_vma=False,
    )
```

```python
import functools

import jax
import jax.numpy as jnp
from jax import lax
from jax.experimental import pallas as pl
from jax.experimental.pallas import tpu as pltpu
from jax.sharding import PartitionSpec as P

M = 1280
FACE = 192
ANG = 512
EXC = 128
PADDED = 256
CHUNKS = 5
ROWS = M // CHUNKS
PARTS = 4
PART_ROWS = ANG // PARTS
BLOCK = 64
MESH = pl.DeviceIdType.MESH
PICK_ORDER = (4, 0, 1, 2, 3, 5)
TAKE_ORDER = (2, 0, 1)
BF16, F32 = jnp.bfloat16, jnp.float32


def plane_order():
    steps = [(a, b, c) for a in range(2) for b in range(4) for c in range(2) if (a, b, c) != (0, 0, 0)]
    return sorted(steps, key=lambda s: -((2 if s[1] == 2 else s[1] % 2) + (1 if s[2] else 2 * s[0])))


def kernel(
    incident, response, radiation, face_index, linked, out_ref,
    inc, resp, rad, slots_raw, slots, link, select, place, weights, outgoing, sent, near_in, far_in, total, columns, field,
    keep, half_out, half_in, plane_out, plane_in, line_out, line_in,
    load_sem, resp_sem, face_send, face_recv, half_send, half_recv, plane_send, plane_recv, line_send, line_recv,
):
    loads = [
        pltpu.make_async_copy(face_index, slots_raw, load_sem.at[0]),
        pltpu.make_async_copy(incident, inc, load_sem.at[1]),
        pltpu.make_async_copy(linked, link, load_sem.at[2]),
    ]
    for load in loads:
        load.start()
    resp_loads = []
    for c in range(CHUNKS):
        rows = pl.ds(c * ROWS, ROWS)
        pair = [
            pltpu.make_async_copy(response.at[p, rows], resp.at[rows, pl.ds(p * M, M)], resp_sem.at[c, p])
            for p in range(2)
        ]
        resp_loads.append(pair)

    def start_response(c):
        for load in resp_loads[c]:
            load.start()

    start_response(0)
    start_response(1)
    rad_loads = [
        pltpu.make_async_copy(radiation.at[p], rad.at[:, pl.ds(p * M, M)], load_sem.at[3 + p]) for p in range(2)
    ]

    gx, gy, gz = lax.axis_index("gx"), lax.axis_index("gy"), lax.axis_index("gz")
    core, y_lo = gy % 2, gy // 2
    x, y_hi = gz % 4, gz // 4
    me_plane = gz * 2 + y_lo

    near_in[...] = jnp.zeros_like(near_in)
    for g in range(3):
        far_in[g, 0 : 2 * PADDED] = jnp.zeros((2 * PADDED, 2 * EXC), BF16)
    plane_in[...] = jnp.zeros_like(plane_in)
    line_in[...] = jnp.zeros_like(line_in)

    barrier = pltpu.get_barrier_semaphore()

    def greet(device):
        pl.semaphore_signal(barrier, inc=1, device_id=device, device_id_type=MESH)

    def plane_peer(step):
        dyh, dx, dyl = step
        peer_gz = ((y_hi + dyh) % 2) * 4 + (x + dx) % 4
        peer_lo = (y_lo + dyl) % 2
        return peer_gz * 2 + peer_lo, (gx, peer_lo * 2 + core, peer_gz)

    order = plane_order()
    partner = (gx, gy + 1 - 2 * core, gz)
    cross = (gx, 3 - gy, gz)
    middle = (gy + 1) // 2 == 1
    for step in order:
        greet(plane_peer(step)[1])
    for d in range(1, 8):
        greet(((gx + d) % 8, gy, gz))
    greet(partner)

    @pl.when(middle)
    def _():
        greet(cross)

    ahead, across = core, 1 - core
    face_of = (4 * ahead, 4 * ahead + 1, 4 * across, 4 * across + 1, 2 + core, 3 - core)
    place_a, place_b = gx * across + gz * ahead, gx * ahead + gz * across
    there = (place_a > 0, place_a < 7, place_b > 0, place_b < 7, middle, None)
    target = (
        (gx - across, gy, gz - ahead),
        (gx + across, gy, gz + ahead),
        (gx - ahead, gy, gz - across),
        (gx + ahead, gy, gz + across),
        cross,
        partner,
    )
    landing = (1, 0, 3, 2, 4, 5)

    def guarded(role, action):
        if there[role] is None:
            action()
        else:
            pl.when(there[role])(action)

    slots[...] = jnp.full(slots.shape, -1, jnp.int32)
    loads[0].wait()
    for f in range(6):
        slots[f : f + 1, 0:FACE] = slots_raw[f]
    lanes128 = lax.broadcasted_iota(jnp.int32, (128, 128), 1).astype(F32)
    for r in PICK_ORDER:
        row = slots[pl.ds(face_of[r], 1), :].astype(F32)
        for half, count in ((0, 128), (1, 64)):
            wide = jnp.broadcast_to(row[:, half * 128 : (half + 1) * 128], (128, 128))
            tall = jnp.transpose(wide)[:count]
            for c in range(M // 128):
                hit = tall - float(c * 128) == lanes128[:count]
                select[r, half * 128 : half * 128 + count, c * 128 : (c + 1) * 128] = jnp.where(hit, 1.0, 0.0).astype(BF16)

    def set_weights(rows, real, imag):
        low = pl.ds(rows.start, rows.size)
        high = pl.ds(M + rows.start, rows.size)
        weights[low, 0:EXC] = real
        weights[low, EXC : 2 * EXC] = imag
        weights[high, 0:EXC] = -imag
        weights[high, EXC : 2 * EXC] = real

    start_response(2)
    loads[1].wait()
    for c in range(CHUNKS):
        rows = pl.ds(c * ROWS, ROWS)
        set_weights(rows, inc[0, rows], inc[1, rows])

    def respond(first):
        for c in range(CHUNKS):
            rows = pl.ds(c * ROWS, ROWS)
            if first:
                for load in resp_loads[c]:
                    load.wait()
                if c + 3 < CHUNKS:
                    start_response(c + 3)
                if c + 3 == CHUNKS:
                    for load in rad_loads:
                        load.start()
            outgoing[rows] = jnp.dot(resp[rows], weights[...], preferred_element_type=F32).astype(BF16)

    def into(it, spot):
        if it == 0:
            return near_in.at[pl.ds(spot * PADDED, FACE)]
        return far_in.at[spot // 2, pl.ds((spot % 2) * PADDED, FACE)]

    def face_copy(it, role, spot, device):
        return pltpu.make_async_remote_copy(
            src_ref=sent.at[it, role],
            dst_ref=into(it, spot),
            send_sem=face_send.at[it, role],
            recv_sem=face_recv.at[it, spot],
            device_id=device,
            device_id_type=MESH,
        )

    crossing = jnp.where((gz == 3) | (gz == 4), 1, 0)
    far = 2 * across + jnp.where(gz == 3, 1, 0)
    sequence = [
        usual + crossing * (other - usual)
        for usual, other in zip(PICK_ORDER, (far, 4, (far + 1) % 4, (far + 2) % 4, (far + 3) % 4))
    ]

    def send_faces(it):
        for r in sequence:
            sent[it, r] = jnp.dot(select[r], outgoing[...], preferred_element_type=F32).astype(BF16)
            line = jnp.where(r < 4, 1, 0)
            up = r % 2
            along_z = (r // 2 + core + 1) % 2 * line
            along_x = (r // 2 + core) % 2 * line
            move = 2 * up - 1
            device = (gx + along_z * move, gy + (1 - line) * (3 - 2 * gy), gz + along_x * move)
            at = gx * along_z + gz * along_x
            last = 7 * up
            inside = ((r < 4) & (at != last)) | ((r == 4) & middle)
            spot = r + line * (1 - 2 * up)
            pl.when(inside)(face_copy(it, r, spot, device).start)
        sent[it, 5] = jnp.dot(select[5], outgoing[...], preferred_element_type=F32).astype(BF16)
        face_copy(it, 5, 5, partner).start()

    def take_faces(it, roles):
        for r in roles:
            guarded(r, face_copy(it, r, r, target[r]).wait_recv)

    def add_traces():
        for n, g in enumerate(TAKE_ORDER):
            take_faces(0, (2 * g, 2 * g + 1))
            span = slice(2 * g * PADDED, (2 * g + 2) * PADDED)
            for c in range(CHUNKS):
                rows = pl.ds(c * ROWS, ROWS)
                trace = jnp.dot(place[rows, span], near_in[span], preferred_element_type=F32)
                if n > 0:
                    trace = trace + total[rows]
                if n < 2:
                    total[rows] = trace
                else:
                    real = (trace[:, 0:EXC] + inc[0, rows].astype(F32)).astype(BF16)
                    imag = (trace[:, EXC : 2 * EXC] + inc[1, rows].astype(F32)).astype(BF16)
                    set_weights(rows, real, imag)

    def gather_columns(g, p):
        picked = jnp.dot(
            rad[:, p * M : (p + 1) * M], place[:, 2 * g * PADDED : (2 * g + 2) * PADDED], preferred_element_type=F32
        )
        columns[g, :, 2 * p * PADDED : (2 * p + 2) * PADDED] = picked.astype(BF16)

    respond(True)
    pl.semaphore_wait(barrier, 15 + 7 + 1 + jnp.where(middle, 1, 0))
    send_faces(0)

    for load in rad_loads:
        load.wait()
    field[...] = jnp.dot(rad[...], weights[...], preferred_element_type=F32)
    loads[2].wait()
    for r in range(6):
        row = jnp.where(link[0, face_of[r]] > 0, slots[pl.ds(face_of[r], 1), :], -1)
        for c in range(CHUNKS):
            spots = lax.broadcasted_iota(jnp.int32, (ROWS, PADDED), 0) + c * ROWS
            place[c * ROWS : (c + 1) * ROWS, r * PADDED : (r + 1) * PADDED] = jnp.where(spots == row, 1.0, 0.0).astype(BF16)
    gather_columns(TAKE_ORDER[0], 0)
    gather_columns(TAKE_ORDER[0], 1)

    add_traces()
    respond(False)
    send_faces(1)
    for g in TAKE_ORDER[1:]:
        gather_columns(g, 0)
        gather_columns(g, 1)

    lanes = lax.broadcasted_iota(jnp.int32, (PART_ROWS, EXC), 1)
    odd_core = (lanes // 4) % 2
    half_copies = []
    for n, g in enumerate(TAKE_ORDER):
        take_faces(1, (2 * g, 2 * g + 1))
        low, high = slice(0, 2 * PADDED), slice(2 * PADDED, 4 * PADDED)
        far_in[g, high, 0:EXC] = -far_in[g, low, EXC : 2 * EXC]
        far_in[g, high, EXC : 2 * EXC] = far_in[g, low, 0:EXC]
        for q in range(PARTS):
            rows = pl.ds(q * PART_ROWS, PART_ROWS)
            value = field[rows] + jnp.dot(columns[g, rows], far_in[g], preferred_element_type=F32)
            if n < 2:
                field[rows] = value
                continue
            real, imag = value[:, 0:EXC], value[:, EXC : 2 * EXC]
            zero = jnp.where(odd_core == 0, real, pltpu.roll(imag, 4, 1))
            one = jnp.where(odd_core == 0, pltpu.roll(real, EXC - 4, 1), imag)
            keep[rows] = jnp.where(core == 0, zero, one)
            half_out[rows] = jnp.where(core == 0, one, zero)
            copy = pltpu.make_async_remote_copy(
                src_ref=half_out.at[rows],
                dst_ref=half_in.at[rows],
                send_sem=half_send.at[q],
                recv_sem=half_recv.at[q],
                device_id=partner,
                device_id_type=MESH,
            )
            copy.start()
            half_copies.append(copy)

    small = lax.broadcasted_iota(jnp.int32, (BLOCK // 2, EXC), 1)
    odd_lo = (small // 8) % 2
    for q in range(PARTS):
        half_copies[q].wait_recv()
        for b in range(PART_ROWS // BLOCK):
            start = q * PART_ROWS + b * BLOCK
            first = pl.ds(start, BLOCK // 2)
            second = pl.ds(start + BLOCK // 2, BLOCK // 2)
            top = keep[first] + half_in[first]
            low = keep[second] + half_in[second]
            slot = (q * (PART_ROWS // BLOCK) + b) * 2
            plane_out[slot] = jnp.where(odd_lo == 0, top, pltpu.roll(low, 8, 1)).astype(BF16)
            plane_out[slot + 1] = jnp.where(odd_lo == 0, pltpu.roll(top, EXC - 8, 1), low).astype(BF16)

    plane_copies = []
    for n, step in enumerate(order):
        peer, device = plane_peer(step)
        copy = pltpu.make_async_remote_copy(
            src_ref=plane_out.at[peer],
            dst_ref=plane_in.at[me_plane],
            send_sem=plane_send.at[n],
            recv_sem=plane_recv.at[me_plane],
            device_id=device,
            device_id_type=MESH,
        )
        copy.start()
        plane_copies.append(copy)
    for s in range(16):

        @pl.when(s != me_plane)
        def _():
            pltpu.make_async_remote_copy(
                src_ref=plane_out.at[s],
                dst_ref=plane_in.at[s],
                send_sem=plane_send.at[0],
                recv_sem=plane_recv.at[s],
                device_id=partner,
                device_id_type=MESH,
            ).wait_recv()

    piece = plane_out[me_plane].astype(F32)
    for s in range(16):
        piece = piece + plane_in[s].astype(F32)
    tall = jnp.concatenate([piece, pltpu.roll(piece, EXC - 8, 1)], axis=0)
    turned = jnp.transpose(jnp.concatenate([tall, tall], axis=0))
    for d in range(8):
        line_out[d] = turned[d * 16 : d * 16 + 8]
    line_copies = []
    for d in (4, 3, 5, 2, 6, 1, 7):
        peer = (gx + d) % 8
        copy = pltpu.make_async_remote_copy(
            src_ref=line_out.at[peer],
            dst_ref=line_in.at[gx],
            send_sem=line_send.at[d],
            recv_sem=line_recv.at[gx],
            device_id=(peer, gy, gz),
            device_id_type=MESH,
        )
        copy.start()
        line_copies.append(copy)

    for it in range(2):
        for r in range(6):
            guarded(r, face_copy(it, r, landing[r], target[r]).wait_send)
    for copy in half_copies + plane_copies:
        copy.wait_send()

    for s in range(8):

        @pl.when(s != gx)
        def _():
            pltpu.make_async_remote_copy(
                src_ref=line_out.at[s],
                dst_ref=line_in.at[s],
                send_sem=line_send.at[0],
                recv_sem=line_recv.at[s],
                device_id=partner,
                device_id_type=MESH,
            ).wait_recv()

    result = line_out[gx]
    for s in range(8):
        result = result + line_in[s]
    out_ref[0] = result[0:4, 0:BLOCK]
    out_ref[1] = result[4:8, 0:BLOCK]
    for copy in line_copies:
        copy.wait_send()


def shards(incident, response, radiation, face_index, linked):
    anywhere = pl.BlockSpec(memory_space=pl.ANY)
    dma = pltpu.SemaphoreType.DMA
    return pl.pallas_call(
        kernel,
        out_shape=pltpu.VMEM((2, 4, BLOCK), F32),
        in_specs=[anywhere] * 5,
        out_specs=pl.BlockSpec(memory_space=pltpu.VMEM),
        scratch_shapes=[
            pltpu.VMEM((2, M, EXC), BF16),
            pltpu.VMEM((M, 2 * M), BF16),
            pltpu.VMEM((ANG, 2 * M), BF16),
            pltpu.VMEM((6, 1, FACE), jnp.int32),
            pltpu.VMEM((8, PADDED), jnp.int32),
            pltpu.SMEM((1, 6), jnp.int32),
            pltpu.VMEM((6, FACE, M), BF16),
            pltpu.VMEM((M, 6 * PADDED), BF16),
            pltpu.VMEM((2 * M, 2 * EXC), BF16),
            pltpu.VMEM((M, 2 * EXC), BF16),
            pltpu.VMEM((2, 6, FACE, 2 * EXC), BF16),
            pltpu.VMEM((6 * PADDED, 2 * EXC), BF16),
            pltpu.VMEM((3, 4 * PADDED, 2 * EXC), BF16),
            pltpu.VMEM((M, 2 * EXC), F32),
            pltpu.VMEM((3, ANG, 4 * PADDED), BF16),
            pltpu.VMEM((ANG, 2 * EXC), F32),
            pltpu.VMEM((ANG, EXC), F32),
            pltpu.VMEM((ANG, EXC), F32),
            pltpu.VMEM((ANG, EXC), F32),
            pltpu.VMEM((16, BLOCK // 2, EXC), BF16),
            pltpu.VMEM((16, BLOCK // 2, EXC), BF16),
            pltpu.VMEM((8, 8, EXC), F32),
            pltpu.VMEM((8, 8, EXC), F32),
            dma((5,)),
            dma((CHUNKS, 2)),
            dma((2, 6)),
            dma((2, 6)),
            dma((PARTS,)),
            dma((PARTS,)),
            dma((16,)),
            dma((16,)),
            dma((8,)),
            dma((8,)),
        ],
        compiler_params=pltpu.CompilerParams(
            collective_id=0, has_side_effects=True, vmem_limit_bytes=60 * 1024 * 1024
        ),
        cost_estimate=pl.CostEstimate(flops=8_000_000_000, bytes_accessed=10_000_000, transcendentals=0),
        name="schwarz",
    )(
        incident.reshape(2, M, EXC),
        response.reshape(2, M, M),
        radiation.reshape(2, ANG, M),
        face_index.reshape(6, 1, FACE),
        linked.reshape(1, 6),
    )


def solution(mesh):
    return jax.shard_map(
        shards,
        mesh=mesh,
        in_specs=(
            P("gx", "gy", "gz", None, None, None),
            P("gx", "gy", "gz", None, None, None),
            P("gx", "gy", "gz", None, None, None),
            P("gx", "gy", "gz", None, None),
            P("gx", "gy", "gz", None),
        ),
        out_specs=P(None, ("gx", "gy"), "gz"),
        check_vma=False,
    )
```

```python
import functools

import jax
import jax.numpy as jnp
from jax import lax
from jax.experimental import pallas as pl
from jax.experimental.pallas import tpu as pltpu
from jax.sharding import PartitionSpec as P

M = 1280
FACE = 192
ANG = 512
EXC = 128
PADDED = 256
CHUNKS = 5
ROWS = M // CHUNKS
PARTS = 4
PART_ROWS = ANG // PARTS
BLOCK = 64
MESH = pl.DeviceIdType.MESH
TAKE_ORDER = (2, 0, 1)
BF16, F32 = jnp.bfloat16, jnp.float32


def plane_order():
    steps = [(a, b, c) for a in range(2) for b in range(4) for c in range(2) if (a, b, c) != (0, 0, 0)]
    return sorted(steps, key=lambda s: -((2 if s[1] == 2 else s[1] % 2) + (1 if s[2] else 2 * s[0])))


def kernel(
    incident, response, radiation, face_index, linked, out_ref,
    inc, resp, rad, slots_raw, slots, link, select, place, weights, outgoing, sent, near_in, far_in, total, columns, field,
    keep, half_out, half_in, plane_out, plane_in, line_out, line_in,
    load_sem, resp_sem, face_send, face_recv, half_send, half_recv, plane_send, plane_recv, line_send, line_recv,
):
    loads = [
        pltpu.make_async_copy(face_index, slots_raw, load_sem.at[0]),
        pltpu.make_async_copy(incident, inc, load_sem.at[1]),
        pltpu.make_async_copy(linked, link, load_sem.at[2]),
    ]
    for load in loads:
        load.start()
    resp_loads = []
    for c in range(CHUNKS):
        rows = pl.ds(c * ROWS, ROWS)
        pair = [
            pltpu.make_async_copy(response.at[p, rows], resp.at[rows, pl.ds(p * M, M)], resp_sem.at[c, p])
            for p in range(2)
        ]
        resp_loads.append(pair)

    def start_response(c):
        for load in resp_loads[c]:
            load.start()

    start_response(0)
    rad_loads = [
        pltpu.make_async_copy(radiation.at[p], rad.at[:, pl.ds(p * M, M)], load_sem.at[3 + p]) for p in range(2)
    ]

    gx, gy, gz = lax.axis_index("gx"), lax.axis_index("gy"), lax.axis_index("gz")
    core, y_lo = gy % 2, gy // 2
    x, y_hi = gz % 4, gz // 4
    me_plane = gz * 2 + y_lo

    near_in[...] = jnp.zeros_like(near_in)
    for g in range(3):
        far_in[g, 0 : 2 * PADDED] = jnp.zeros((2 * PADDED, 2 * EXC), BF16)
    plane_in[...] = jnp.zeros_like(plane_in)
    line_in[...] = jnp.zeros_like(line_in)

    barrier = pltpu.get_barrier_semaphore()

    def greet(device):
        pl.semaphore_signal(barrier, inc=1, device_id=device, device_id_type=MESH)

    def plane_peer(step):
        dyh, dx, dyl = step
        peer_gz = ((y_hi + dyh) % 2) * 4 + (x + dx) % 4
        peer_lo = (y_lo + dyl) % 2
        return peer_gz * 2 + peer_lo, (gx, peer_lo * 2 + core, peer_gz)

    order = plane_order()
    partner = (gx, gy + 1 - 2 * core, gz)
    cross = (gx, 3 - gy, gz)
    middle = (gy + 1) // 2 == 1
    for step in order:
        greet(plane_peer(step)[1])
    for d in range(1, 8):
        greet(((gx + d) % 8, gy, gz))
    greet(partner)

    @pl.when(middle)
    def _():
        greet(cross)

    start_response(1)

    ahead, across = core, 1 - core
    face_of = (4 * ahead, 4 * ahead + 1, 4 * across, 4 * across + 1, 2 + core, 3 - core)
    place_a, place_b = gx * across + gz * ahead, gx * ahead + gz * across
    there = (place_a > 0, place_a < 7, place_b > 0, place_b < 7, middle, None)
    target = (
        (gx - across, gy, gz - ahead),
        (gx + across, gy, gz + ahead),
        (gx - ahead, gy, gz - across),
        (gx + ahead, gy, gz + across),
        cross,
        partner,
    )
    landing = (1, 0, 3, 2, 4, 5)

    def guarded(role, action):
        if there[role] is None:
            action()
        else:
            pl.when(there[role])(action)

    slots[...] = jnp.full(slots.shape, -1, jnp.int32)
    loads[0].wait()
    for f in range(6):
        slots[f : f + 1, 0:FACE] = slots_raw[f]
    lanes128 = lax.broadcasted_iota(jnp.int32, (128, 128), 1).astype(F32)
    for r in range(6):
        row = slots[pl.ds(face_of[r], 1), :].astype(F32)
        for half, count in ((0, 128), (1, 64)):
            wide = jnp.broadcast_to(row[:, half * 128 : (half + 1) * 128], (128, 128))
            tall = jnp.transpose(wide)[:count]
            for c in range(M // 128):
                hit = tall - float(c * 128) == lanes128[:count]
                start = (r % 2) * FACE + half * 128
                select[r // 2, start : start + count, c * 128 : (c + 1) * 128] = jnp.where(hit, 1.0, 0.0).astype(BF16)

    def set_weights(rows, real, imag):
        low = pl.ds(rows.start, rows.size)
        high = pl.ds(M + rows.start, rows.size)
        weights[low, 0:EXC] = real
        weights[low, EXC : 2 * EXC] = imag
        weights[high, 0:EXC] = -imag
        weights[high, EXC : 2 * EXC] = real

    start_response(2)
    loads[1].wait()
    for c in range(CHUNKS):
        rows = pl.ds(c * ROWS, ROWS)
        set_weights(rows, inc[0, rows], inc[1, rows])

    def respond(first):
        for c in range(CHUNKS):
            rows = pl.ds(c * ROWS, ROWS)
            if first:
                for load in resp_loads[c]:
                    load.wait()
                if c + 3 < CHUNKS:
                    start_response(c + 3)
                if c + 3 == CHUNKS:
                    for load in rad_loads:
                        load.start()
            outgoing[rows] = jnp.dot(resp[rows], weights[...], preferred_element_type=F32).astype(BF16)

    def into(it, spot):
        if it == 0:
            return near_in.at[pl.ds(spot * PADDED, FACE)]
        return far_in.at[spot // 2, pl.ds((spot % 2) * PADDED, FACE)]

    def face_copy(it, role, spot, device):
        return pltpu.make_async_remote_copy(
            src_ref=sent.at[it, role],
            dst_ref=into(it, spot),
            send_sem=face_send.at[it, role],
            recv_sem=face_recv.at[it, spot],
            device_id=device,
            device_id_type=MESH,
        )

    early = across * jnp.where((gz == 3) | (gz == 4), 1, 0)

    def send_faces(it):
        for g in (early, 1 - early, 2):
            picked = jnp.dot(select[g], outgoing[...], preferred_element_type=F32).astype(BF16)
            for up in range(2):
                sent[it, 2 * g + up] = picked[up * FACE : (up + 1) * FACE]
            if isinstance(g, int):
                pl.when(middle)(face_copy(it, 4, 4, cross).start)
                face_copy(it, 5, 5, partner).start()
                continue
            along_x = (g + core) % 2
            along_z = 1 - along_x
            at = gx * along_z + gz * along_x
            for up in range(2):
                move = 2 * up - 1
                device = (gx + along_z * move, gy, gz + along_x * move)
                pl.when(at != 7 * up)(face_copy(it, 2 * g + up, 2 * g + 1 - up, device).start)

    def take_faces(it, roles):
        for r in roles:
            guarded(r, face_copy(it, r, r, target[r]).wait_recv)

    def add_traces():
        for n, g in enumerate(TAKE_ORDER):
            take_faces(0, (2 * g, 2 * g + 1))
            span = slice(2 * g * PADDED, (2 * g + 2) * PADDED)
            for c in range(CHUNKS):
                rows = pl.ds(c * ROWS, ROWS)
                trace = jnp.dot(place[rows, span], near_in[span], preferred_element_type=F32)
                if n > 0:
                    trace = trace + total[rows]
                if n < 2:
                    total[rows] = trace
                else:
                    real = (trace[:, 0:EXC] + inc[0, rows].astype(F32)).astype(BF16)
                    imag = (trace[:, EXC : 2 * EXC] + inc[1, rows].astype(F32)).astype(BF16)
                    set_weights(rows, real, imag)

    def gather_columns(g, p):
        picked = jnp.dot(
            rad[:, p * M : (p + 1) * M], place[:, 2 * g * PADDED : (2 * g + 2) * PADDED], preferred_element_type=F32
        )
        columns[g, :, 2 * p * PADDED : (2 * p + 2) * PADDED] = picked.astype(BF16)

    respond(True)
    pl.semaphore_wait(barrier, 15 + 7 + 1 + jnp.where(middle, 1, 0))
    send_faces(0)

    for load in rad_loads:
        load.wait()
    field[...] = jnp.dot(rad[...], weights[...], preferred_element_type=F32)
    loads[2].wait()
    for r in range(6):
        row = jnp.where(link[0, face_of[r]] > 0, slots[pl.ds(face_of[r], 1), :], -1)
        for c in range(CHUNKS):
            spots = lax.broadcasted_iota(jnp.int32, (ROWS, PADDED), 0) + c * ROWS
            place[c * ROWS : (c + 1) * ROWS, r * PADDED : (r + 1) * PADDED] = jnp.where(spots == row, 1.0, 0.0).astype(BF16)
    gather_columns(TAKE_ORDER[0], 0)
    gather_columns(TAKE_ORDER[0], 1)

    add_traces()
    respond(False)
    send_faces(1)
    for g in TAKE_ORDER[1:]:
        gather_columns(g, 0)
        gather_columns(g, 1)

    lanes = lax.broadcasted_iota(jnp.int32, (PART_ROWS, EXC), 1)
    odd_core = (lanes // 4) % 2
    half_copies = []
    for n, g in enumerate(TAKE_ORDER):
        take_faces(1, (2 * g, 2 * g + 1))
        low, high = slice(0, 2 * PADDED), slice(2 * PADDED, 4 * PADDED)
        far_in[g, high, 0:EXC] = -far_in[g, low, EXC : 2 * EXC]
        far_in[g, high, EXC : 2 * EXC] = far_in[g, low, 0:EXC]
        for q in range(PARTS):
            rows = pl.ds(q * PART_ROWS, PART_ROWS)
            value = field[rows] + jnp.dot(columns[g, rows], far_in[g], preferred_element_type=F32)
            if n < 2:
                field[rows] = value
                continue
            real, imag = value[:, 0:EXC], value[:, EXC : 2 * EXC]
            zero = jnp.where(odd_core == 0, real, pltpu.roll(imag, 4, 1))
            one = jnp.where(odd_core == 0, pltpu.roll(real, EXC - 4, 1), imag)
            keep[rows] = jnp.where(core == 0, zero, one)
            half_out[rows] = jnp.where(core == 0, one, zero)
            copy = pltpu.make_async_remote_copy(
                src_ref=half_out.at[rows],
                dst_ref=half_in.at[rows],
                send_sem=half_send.at[q],
                recv_sem=half_recv.at[q],
                device_id=partner,
                device_id_type=MESH,
            )
            copy.start()
            half_copies.append(copy)

    small = lax.broadcasted_iota(jnp.int32, (BLOCK // 2, EXC), 1)
    odd_lo = (small // 8) % 2
    for q in range(PARTS):
        half_copies[q].wait_recv()
        for b in range(PART_ROWS // BLOCK):
            start = q * PART_ROWS + b * BLOCK
            first = pl.ds(start, BLOCK // 2)
            second = pl.ds(start + BLOCK // 2, BLOCK // 2)
            top = keep[first] + half_in[first]
            low = keep[second] + half_in[second]
            slot = (q * (PART_ROWS // BLOCK) + b) * 2
            plane_out[slot] = jnp.where(odd_lo == 0, top, pltpu.roll(low, 8, 1)).astype(BF16)
            plane_out[slot + 1] = jnp.where(odd_lo == 0, pltpu.roll(top, EXC - 8, 1), low).astype(BF16)

    plane_copies = []
    for n, step in enumerate(order):
        peer, device = plane_peer(step)
        copy = pltpu.make_async_remote_copy(
            src_ref=plane_out.at[peer],
            dst_ref=plane_in.at[me_plane],
            send_sem=plane_send.at[n],
            recv_sem=plane_recv.at[me_plane],
            device_id=device,
            device_id_type=MESH,
        )
        copy.start()
        plane_copies.append(copy)
    for s in range(16):

        @pl.when(s != me_plane)
        def _():
            pltpu.make_async_remote_copy(
                src_ref=plane_out.at[s],
                dst_ref=plane_in.at[s],
                send_sem=plane_send.at[0],
                recv_sem=plane_recv.at[s],
                device_id=partner,
                device_id_type=MESH,
            ).wait_recv()

    piece = plane_out[me_plane].astype(F32)
    for s in range(16):
        piece = piece + plane_in[s].astype(F32)
    tall = jnp.concatenate([piece, pltpu.roll(piece, EXC - 8, 1)], axis=0)
    turned = jnp.transpose(jnp.concatenate([tall, tall], axis=0))
    for d in range(8):
        line_out[d] = turned[d * 16 : d * 16 + 8]
    line_copies = []
    for d in (4, 3, 5, 2, 6, 1, 7):
        peer = (gx + d) % 8
        copy = pltpu.make_async_remote_copy(
            src_ref=line_out.at[peer],
            dst_ref=line_in.at[gx],
            send_sem=line_send.at[d],
            recv_sem=line_recv.at[gx],
            device_id=(peer, gy, gz),
            device_id_type=MESH,
        )
        copy.start()
        line_copies.append(copy)

    for it in range(2):
        for r in range(6):
            guarded(r, face_copy(it, r, landing[r], target[r]).wait_send)
    for copy in half_copies + plane_copies:
        copy.wait_send()

    for s in range(8):

        @pl.when(s != gx)
        def _():
            pltpu.make_async_remote_copy(
                src_ref=line_out.at[s],
                dst_ref=line_in.at[s],
                send_sem=line_send.at[0],
                recv_sem=line_recv.at[s],
                device_id=partner,
                device_id_type=MESH,
            ).wait_recv()

    result = line_out[gx]
    for s in range(8):
        result = result + line_in[s]
    out_ref[0] = result[0:4, 0:BLOCK]
    out_ref[1] = result[4:8, 0:BLOCK]
    for copy in line_copies:
        copy.wait_send()


def shards(incident, response, radiation, face_index, linked):
    anywhere = pl.BlockSpec(memory_space=pl.ANY)
    dma = pltpu.SemaphoreType.DMA
    return pl.pallas_call(
        kernel,
        out_shape=pltpu.VMEM((2, 4, BLOCK), F32),
        in_specs=[anywhere] * 5,
        out_specs=pl.BlockSpec(memory_space=pltpu.VMEM),
        scratch_shapes=[
            pltpu.VMEM((2, M, EXC), BF16),
            pltpu.VMEM((M, 2 * M), BF16),
            pltpu.VMEM((ANG, 2 * M), BF16),
            pltpu.VMEM((6, 1, FACE), jnp.int32),
            pltpu.VMEM((8, PADDED), jnp.int32),
            pltpu.SMEM((1, 6), jnp.int32),
            pltpu.VMEM((3, 2 * FACE, M), BF16),
            pltpu.VMEM((M, 6 * PADDED), BF16),
            pltpu.VMEM((2 * M, 2 * EXC), BF16),
            pltpu.VMEM((M, 2 * EXC), BF16),
            pltpu.VMEM((2, 6, FACE, 2 * EXC), BF16),
            pltpu.VMEM((6 * PADDED, 2 * EXC), BF16),
            pltpu.VMEM((3, 4 * PADDED, 2 * EXC), BF16),
            pltpu.VMEM((M, 2 * EXC), F32),
            pltpu.VMEM((3, ANG, 4 * PADDED), BF16),
            pltpu.VMEM((ANG, 2 * EXC), F32),
            pltpu.VMEM((ANG, EXC), F32),
            pltpu.VMEM((ANG, EXC), F32),
            pltpu.VMEM((ANG, EXC), F32),
            pltpu.VMEM((16, BLOCK // 2, EXC), BF16),
            pltpu.VMEM((16, BLOCK // 2, EXC), BF16),
            pltpu.VMEM((8, 8, EXC), F32),
            pltpu.VMEM((8, 8, EXC), F32),
            dma((5,)),
            dma((CHUNKS, 2)),
            dma((2, 6)),
            dma((2, 6)),
            dma((PARTS,)),
            dma((PARTS,)),
            dma((16,)),
            dma((16,)),
            dma((8,)),
            dma((8,)),
        ],
        compiler_params=pltpu.CompilerParams(
            collective_id=0, has_side_effects=True, vmem_limit_bytes=60 * 1024 * 1024
        ),
        cost_estimate=pl.CostEstimate(flops=8_000_000_000, bytes_accessed=10_000_000, transcendentals=0),
        name="schwarz",
    )(
        incident.reshape(2, M, EXC),
        response.reshape(2, M, M),
        radiation.reshape(2, ANG, M),
        face_index.reshape(6, 1, FACE),
        linked.reshape(1, 6),
    )


def solution(mesh):
    return jax.shard_map(
        shards,
        mesh=mesh,
        in_specs=(
            P("gx", "gy", "gz", None, None, None),
            P("gx", "gy", "gz", None, None, None),
            P("gx", "gy", "gz", None, None, None),
            P("gx", "gy", "gz", None, None),
            P("gx", "gy", "gz", None),
        ),
        out_specs=P(None, ("gx", "gy"), "gz"),
        check_vma=False,
    )
```

```python
import functools

import jax
import jax.numpy as jnp
from jax import lax
from jax.experimental import pallas as pl
from jax.experimental.pallas import tpu as pltpu
from jax.sharding import PartitionSpec as P

M = 1280
FACE = 192
ANG = 512
EXC = 128
PADDED = 256
PAIR = 2 * FACE
CHUNKS = 5
ROWS = M // CHUNKS
PARTS = 2
PART_ROWS = ANG // PARTS
BLOCK = 64
MESH = pl.DeviceIdType.MESH
TAKE_ORDER = (2, 0, 1)
BF16, F32 = jnp.bfloat16, jnp.float32


def plane_order():
    steps = [(a, b, c) for a in range(2) for b in range(4) for c in range(2) if (a, b, c) != (0, 0, 0)]
    return sorted(steps, key=lambda s: -((2 if s[1] == 2 else s[1] % 2) + (1 if s[2] else 2 * s[0])))


def kernel(
    incident, response, radiation, face_index, linked, out_ref,
    inc, resp, rad, slots_raw, slots, link, rows_of, select, place, weights, outgoing, sent, split, near_in, far_in, total,
    columns, keep, half_out, half_in, plane_out, plane_in, line_out, line_in,
    load_sem, resp_sem, face_send, face_recv, split_send, split_recv, half_send, half_recv, column_send, column_recv,
    plane_send, plane_recv, line_send, line_recv,
):
    loads = [
        pltpu.make_async_copy(face_index, slots_raw, load_sem.at[0]),
        pltpu.make_async_copy(incident, inc, load_sem.at[1]),
        pltpu.make_async_copy(linked, link, load_sem.at[2]),
    ]
    for load in loads:
        load.start()
    resp_loads = []
    for c in range(CHUNKS):
        rows = pl.ds(c * ROWS, ROWS)
        pair = [
            pltpu.make_async_copy(response.at[p, rows], resp.at[rows, pl.ds(p * M, M)], resp_sem.at[c, p])
            for p in range(2)
        ]
        resp_loads.append(pair)

    def start_response(c):
        for load in resp_loads[c]:
            load.start()

    start_response(0)
    rad_loads = [
        pltpu.make_async_copy(radiation.at[p], rad.at[:, pl.ds(p * M, M)], load_sem.at[3 + p]) for p in range(2)
    ]

    gx, gy, gz = lax.axis_index("gx"), lax.axis_index("gy"), lax.axis_index("gz")
    core, y_lo = gy % 2, gy // 2
    x, y_hi = gz % 4, gz // 4
    me_plane = gz * 2 + y_lo

    near_in[...] = jnp.zeros_like(near_in)
    for s in range(2):
        for g in range(3):
            far_in[s, g, 0:PAIR] = jnp.zeros((PAIR, EXC), BF16)
    plane_in[...] = jnp.zeros_like(plane_in)
    line_in[...] = jnp.zeros_like(line_in)

    barrier = pltpu.get_barrier_semaphore()

    def greet(device):
        pl.semaphore_signal(barrier, inc=1, device_id=device, device_id_type=MESH)

    def plane_peer(step):
        dyh, dx, dyl = step
        peer_gz = ((y_hi + dyh) % 2) * 4 + (x + dx) % 4
        peer_lo = (y_lo + dyl) % 2
        return peer_gz * 2 + peer_lo, (gx, peer_lo * 2 + core, peer_gz)

    order = plane_order()
    partner = (gx, gy + 1 - 2 * core, gz)
    cross = (gx, 3 - gy, gz)
    middle = (gy + 1) // 2 == 1
    for step in order:
        greet(plane_peer(step)[1])
    for d in range(1, 8):
        greet(((gx + d) % 8, gy, gz))
    greet(partner)
    greet(cross)
    for d in (1, 7):
        greet(((gx + d) % 8, gy + 1 - 2 * core, gz))
        greet((gx, gy + 1 - 2 * core, (gz + d) % 8))

    start_response(1)

    ahead, across = core, 1 - core
    face_of = (4 * ahead, 4 * ahead + 1, 4 * across, 4 * across + 1, 2 + core, 3 - core)
    place_a, place_b = gx * across + gz * ahead, gx * ahead + gz * across
    there = (place_a > 0, place_a < 7, place_b > 0, place_b < 7, middle, None)
    target = (
        (gx - across, gy, gz - ahead),
        (gx + across, gy, gz + ahead),
        (gx - ahead, gy, gz - across),
        (gx + ahead, gy, gz + across),
        cross,
        partner,
    )
    landing = (1, 0, 3, 2, 4, 5)

    def guarded(role, action):
        if there[role] is None:
            action()
        else:
            pl.when(there[role])(action)

    slots[...] = jnp.full(slots.shape, -1, jnp.int32)
    loads[0].wait()
    for f in range(6):
        slots[f : f + 1, 0:FACE] = slots_raw[f]
    lanes128 = lax.broadcasted_iota(jnp.int32, (128, 128), 1).astype(F32)
    for r in range(6):
        row = slots[pl.ds(face_of[r], 1), :].astype(F32)
        for half, count in ((0, 128), (1, 64)):
            wide = jnp.broadcast_to(row[:, half * 128 : (half + 1) * 128], (128, 128))
            tall = jnp.transpose(wide)[:count]
            for c in range(M // 128):
                hit = tall - float(c * 128) == lanes128[:count]
                start = (r % 2) * FACE + half * 128
                select[r // 2, start : start + count, c * 128 : (c + 1) * 128] = jnp.where(hit, 1.0, 0.0).astype(BF16)

    def set_weights(rows, real, imag):
        low = pl.ds(rows.start, rows.size)
        high = pl.ds(M + rows.start, rows.size)
        weights[low, 0:EXC] = real
        weights[low, EXC : 2 * EXC] = imag
        weights[high, 0:EXC] = -imag
        weights[high, EXC : 2 * EXC] = real

    start_response(2)
    loads[1].wait()
    for c in range(CHUNKS):
        rows = pl.ds(c * ROWS, ROWS)
        set_weights(rows, inc[0, rows], inc[1, rows])

    def respond(first):
        for c in range(CHUNKS):
            rows = pl.ds(c * ROWS, ROWS)
            if first:
                for load in resp_loads[c]:
                    load.wait()
                if c + 3 < CHUNKS:
                    start_response(c + 3)
                if c + 3 == CHUNKS:
                    for load in rad_loads:
                        load.start()
            outgoing[rows] = jnp.dot(resp[rows], weights[...], preferred_element_type=F32).astype(BF16)

    def face_copy(role, spot, device):
        return pltpu.make_async_remote_copy(
            src_ref=sent.at[role],
            dst_ref=near_in.at[pl.ds(spot * FACE, FACE)],
            send_sem=face_send.at[role],
            recv_sem=face_recv.at[spot],
            device_id=device,
            device_id_type=MESH,
        )

    def split_copy(role, half, into, g, up, device):
        return pltpu.make_async_remote_copy(
            src_ref=split.at[half, role],
            dst_ref=far_in.at[into, g, pl.ds(up * FACE, FACE)],
            send_sem=split_send.at[half, role],
            recv_sem=split_recv.at[into, 2 * g + up],
            device_id=device,
            device_id_type=MESH,
        )

    def halves(value, rows):
        odd = (lax.broadcasted_iota(jnp.int32, (rows, EXC), 1) // 4) % 2
        real, imag = value[:, 0:EXC], value[:, EXC : 2 * EXC]
        zero = jnp.where(odd == 0, real, pltpu.roll(imag, 4, 1))
        one = jnp.where(odd == 0, pltpu.roll(real, EXC - 4, 1), imag)
        return zero, one

    early = across * jnp.where((gz == 3) | (gz == 4), 1, 0)

    def send_faces(it):
        for g in (early, 1 - early, 2):
            picked = jnp.dot(select[g], outgoing[...], preferred_element_type=F32)
            if it == 0:
                rounded = picked.astype(BF16)
                for up in range(2):
                    sent[2 * g + up] = rounded[up * FACE : (up + 1) * FACE]
            else:
                for half, value in enumerate(halves(picked, PAIR)):
                    rounded = value.astype(BF16)
                    for up in range(2):
                        split[half, 2 * g + up] = rounded[up * FACE : (up + 1) * FACE]
            if isinstance(g, int):
                if it == 0:
                    pl.when(middle)(face_copy(4, 4, cross).start)
                    face_copy(5, 5, partner).start()
                else:
                    for half in range(2):
                        pl.when(middle)(split_copy(4, half, across, 2, 0, (gx, (1 - y_lo) * 2 + half, gz)).start)
                    split_copy(5, across, across, 2, 1, partner).start()
                    far_in[across, 2, FACE : 2 * FACE] = split[core, 5]
                continue
            along_x = (g + core) % 2
            along_z = 1 - along_x
            at = gx * along_z + gz * along_x
            for up in range(2):
                move = 2 * up - 1
                inside = at != 7 * up
                if it == 0:
                    device = (gx + along_z * move, gy, gz + along_x * move)
                    pl.when(inside)(face_copy(2 * g + up, 2 * g + 1 - up, device).start)
                    continue
                for half in range(2):
                    device = (gx + along_z * move, y_lo * 2 + half, gz + along_x * move)
                    pl.when(inside)(split_copy(2 * g + up, half, core, g, 1 - up, device).start)

    def take_faces(roles):
        for r in roles:
            guarded(r, face_copy(r, r, target[r]).wait_recv)

    def take_halves(g):
        for s in range(2):
            for up in range(2):
                wait = split_copy(2 * g + up, 0, s, g, up, partner).wait_recv
                if g == 2:
                    pl.when(s == core if up else s != y_lo)(wait)
                else:
                    spot = gx if (g + s) % 2 == 0 else gz
                    pl.when(spot < 7 if up else spot > 0)(wait)

    def add_traces():
        for n, g in enumerate(TAKE_ORDER):
            take_faces((2 * g, 2 * g + 1))
            span = slice(g * PAIR, (g + 1) * PAIR)
            for c in range(CHUNKS):
                rows = pl.ds(c * ROWS, ROWS)
                trace = jnp.dot(place[rows, span], near_in[span], preferred_element_type=F32)
                if n > 0:
                    trace = trace + total[rows]
                if n < 2:
                    total[rows] = trace
                else:
                    real = (trace[:, 0:EXC] + inc[0, rows].astype(F32)).astype(BF16)
                    imag = (trace[:, EXC : 2 * EXC] + inc[1, rows].astype(F32)).astype(BF16)
                    set_weights(rows, real, imag)

    def column_copy(s, g):
        return pltpu.make_async_remote_copy(
            src_ref=columns.at[s, g],
            dst_ref=columns.at[s, g],
            send_sem=column_send.at[g],
            recv_sem=column_recv.at[g],
            device_id=partner,
            device_id_type=MESH,
        )

    def gather_columns(g):
        for p in range(2):
            picked = jnp.dot(
                rad[:, p * M : (p + 1) * M], place[:, g * PAIR : (g + 1) * PAIR], preferred_element_type=F32
            )
            columns[core, g, :, p * PAIR : (p + 1) * PAIR] = picked.astype(BF16)
        column_copy(core, g).start()

    respond(True)
    pl.semaphore_wait(barrier, 15 + 7 + 2 + 4)
    send_faces(0)

    for load in rad_loads:
        load.wait()
    half_copies = []
    for q in range(PARTS):
        rows = pl.ds(q * PART_ROWS, PART_ROWS)
        zero, one = halves(jnp.dot(rad[rows], weights[...], preferred_element_type=F32), PART_ROWS)
        keep[rows] = jnp.where(core == 0, zero, one)
        half_out[rows] = jnp.where(core == 0, one, zero)
        half_copies.append(
            pltpu.make_async_remote_copy(
                src_ref=half_out.at[rows],
                dst_ref=half_in.at[rows],
                send_sem=half_send.at[q],
                recv_sem=half_recv.at[q],
                device_id=partner,
                device_id_type=MESH,
            )
        )
        half_copies[q].start()
    loads[2].wait()
    for r in range(6):
        row = jnp.where(link[0, face_of[r]] > 0, slots_raw[face_of[r]], -1)
        rows_of[r // 2 : r // 2 + 1, (r % 2) * FACE : (r % 2 + 1) * FACE] = row
    for g in range(3):
        row = rows_of[g : g + 1, :]
        for c in range(CHUNKS):
            spots = lax.broadcasted_iota(jnp.int32, (ROWS, PAIR), 0) + c * ROWS
            place[c * ROWS : (c + 1) * ROWS, g * PAIR : (g + 1) * PAIR] = jnp.where(spots == row, 1.0, 0.0).astype(BF16)
    gather_columns(TAKE_ORDER[0])

    add_traces()
    respond(False)
    send_faces(1)
    for g in TAKE_ORDER[1:]:
        gather_columns(g)

    odd_part = (lax.broadcasted_iota(jnp.int32, (PAIR, EXC), 1) // 4) % 2
    small = lax.broadcasted_iota(jnp.int32, (BLOCK // 2, EXC), 1)
    odd_lo = (small // 8) % 2
    for copy in half_copies:
        copy.wait_recv()
    for n, g in enumerate(TAKE_ORDER):
        column_copy(across, g).wait_recv()
        take_halves(g)
        for s in range(2):
            faces = far_in[s, g, 0:PAIR].astype(F32)
            turned = jnp.where(odd_part == 0, -pltpu.roll(faces, EXC - 4, 1), pltpu.roll(faces, 4, 1))
            far_in[s, g, PAIR : 2 * PAIR] = turned.astype(BF16)
        for q in range(PARTS):
            rows = pl.ds(q * PART_ROWS, PART_ROWS)
            value = keep[rows]
            if n == 0:
                value = value + half_in[rows]
            for s in range(2):
                value = value + jnp.dot(columns[s, g, rows], far_in[s, g], preferred_element_type=F32)
            if n < 2:
                keep[rows] = value
                continue
            for b in range(PART_ROWS // BLOCK):
                top = value[b * BLOCK : b * BLOCK + BLOCK // 2]
                low = value[b * BLOCK + BLOCK // 2 : (b + 1) * BLOCK]
                slot = (q * (PART_ROWS // BLOCK) + b) * 2
                plane_out[slot] = jnp.where(odd_lo == 0, top, pltpu.roll(low, 8, 1)).astype(BF16)
                plane_out[slot + 1] = jnp.where(odd_lo == 0, pltpu.roll(top, EXC - 8, 1), low).astype(BF16)

    plane_copies = []
    for n, step in enumerate(order):
        peer, device = plane_peer(step)
        copy = pltpu.make_async_remote_copy(
            src_ref=plane_out.at[peer],
            dst_ref=plane_in.at[me_plane],
            send_sem=plane_send.at[n],
            recv_sem=plane_recv.at[me_plane],
            device_id=device,
            device_id_type=MESH,
        )
        copy.start()
        plane_copies.append(copy)
    for s in range(16):

        @pl.when(s != me_plane)
        def _():
            pltpu.make_async_remote_copy(
                src_ref=plane_out.at[s],
                dst_ref=plane_in.at[s],
                send_sem=plane_send.at[0],
                recv_sem=plane_recv.at[s],
                device_id=partner,
                device_id_type=MESH,
            ).wait_recv()

    piece = plane_out[me_plane].astype(F32)
    for s in range(16):
        piece = piece + plane_in[s].astype(F32)
    tall = jnp.concatenate([piece, pltpu.roll(piece, EXC - 8, 1)], axis=0)
    turned = jnp.transpose(jnp.concatenate([tall, tall], axis=0))
    for d in range(8):
        line_out[d] = turned[d * 16 : d * 16 + 8]
    line_copies = []
    for d in (4, 3, 5, 2, 6, 1, 7):
        peer = (gx + d) % 8
        copy = pltpu.make_async_remote_copy(
            src_ref=line_out.at[peer],
            dst_ref=line_in.at[gx],
            send_sem=line_send.at[d],
            recv_sem=line_recv.at[gx],
            device_id=(peer, gy, gz),
            device_id_type=MESH,
        )
        copy.start()
        line_copies.append(copy)

    for r in range(6):
        guarded(r, face_copy(r, landing[r], target[r]).wait_send)
        for half in range(2):
            if r < 5:
                guarded(r, split_copy(r, half, 0, 0, 0, target[r]).wait_send)
    split_copy(5, across, 0, 0, 0, partner).wait_send()
    for g in range(3):
        column_copy(core, g).wait_send()
    for copy in half_copies + plane_copies:
        copy.wait_send()

    for s in range(8):

        @pl.when(s != gx)
        def _():
            pltpu.make_async_remote_copy(
                src_ref=line_out.at[s],
                dst_ref=line_in.at[s],
                send_sem=line_send.at[0],
                recv_sem=line_recv.at[s],
                device_id=partner,
                device_id_type=MESH,
            ).wait_recv()

    result = line_out[gx]
    for s in range(8):
        result = result + line_in[s]
    out_ref[0] = result[0:4, 0:BLOCK]
    out_ref[1] = result[4:8, 0:BLOCK]
    for copy in line_copies:
        copy.wait_send()


def shards(incident, response, radiation, face_index, linked):
    anywhere = pl.BlockSpec(memory_space=pl.ANY)
    dma = pltpu.SemaphoreType.DMA
    return pl.pallas_call(
        kernel,
        out_shape=pltpu.VMEM((2, 4, BLOCK), F32),
        in_specs=[anywhere] * 5,
        out_specs=pl.BlockSpec(memory_space=pltpu.VMEM),
        scratch_shapes=[
            pltpu.VMEM((2, M, EXC), BF16),
            pltpu.VMEM((M, 2 * M), BF16),
            pltpu.VMEM((ANG, 2 * M), BF16),
            pltpu.VMEM((6, 1, FACE), jnp.int32),
            pltpu.VMEM((8, PADDED), jnp.int32),
            pltpu.SMEM((1, 6), jnp.int32),
            pltpu.VMEM((8, PAIR), jnp.int32),
            pltpu.VMEM((3, PAIR, M), BF16),
            pltpu.VMEM((M, 3 * PAIR), BF16),
            pltpu.VMEM((2 * M, 2 * EXC), BF16),
            pltpu.VMEM((M, 2 * EXC), BF16),
            pltpu.VMEM((6, FACE, 2 * EXC), BF16),
            pltpu.VMEM((2, 6, FACE, EXC), BF16),
            pltpu.VMEM((3 * PAIR, 2 * EXC), BF16),
            pltpu.VMEM((2, 3, 2 * PAIR, EXC), BF16),
            pltpu.VMEM((M, 2 * EXC), F32),
            pltpu.VMEM((2, 3, ANG, 2 * PAIR), BF16),
            pltpu.VMEM((ANG, EXC), F32),
            pltpu.VMEM((ANG, EXC), F32),
            pltpu.VMEM((ANG, EXC), F32),
            pltpu.VMEM((16, BLOCK // 2, EXC), BF16),
            pltpu.VMEM((16, BLOCK // 2, EXC), BF16),
            pltpu.VMEM((8, 8, EXC), F32),
            pltpu.VMEM((8, 8, EXC), F32),
            dma((5,)),
            dma((CHUNKS, 2)),
            dma((6,)),
            dma((6,)),
            dma((2, 6)),
            dma((2, 6)),
            dma((PARTS,)),
            dma((PARTS,)),
            dma((3,)),
            dma((3,)),
            dma((16,)),
            dma((16,)),
            dma((8,)),
            dma((8,)),
        ],
        compiler_params=pltpu.CompilerParams(
            collective_id=0, has_side_effects=True, vmem_limit_bytes=60 * 1024 * 1024
        ),
        cost_estimate=pl.CostEstimate(flops=8_000_000_000, bytes_accessed=10_000_000, transcendentals=0),
        name="schwarz",
    )(
        incident.reshape(2, M, EXC),
        response.reshape(2, M, M),
        radiation.reshape(2, ANG, M),
        face_index.reshape(6, 1, FACE),
        linked.reshape(1, 6),
    )


def solution(mesh):
    return jax.shard_map(
        shards,
        mesh=mesh,
        in_specs=(
            P("gx", "gy", "gz", None, None, None),
            P("gx", "gy", "gz", None, None, None),
            P("gx", "gy", "gz", None, None, None),
            P("gx", "gy", "gz", None, None),
            P("gx", "gy", "gz", None),
        ),
        out_specs=P(None, ("gx", "gy"), "gz"),
        check_vma=False,
    )
```

```python
import functools

import jax
import jax.numpy as jnp
from jax import lax
from jax.experimental import pallas as pl
from jax.experimental.pallas import tpu as pltpu
from jax.sharding import PartitionSpec as P

M = 1280
FACE = 192
ANG = 512
EXC = 128
PADDED = 256
PAIR = 2 * FACE
CHUNKS = 5
ROWS = M // CHUNKS
PARTS = 2
PART_ROWS = ANG // PARTS
BLOCK = 64
MESH = pl.DeviceIdType.MESH
TAKE_ORDER = (0, 2, 1)
BF16, F32 = jnp.bfloat16, jnp.float32


def plane_order():
    steps = [(a, b, c) for a in range(2) for b in range(4) for c in range(2) if (a, b, c) != (0, 0, 0)]
    return sorted(steps, key=lambda s: -((2 if s[1] == 2 else s[1] % 2) + (1 if s[2] else 2 * s[0])))


def kernel(
    incident, response, radiation, face_index, linked, out_ref,
    inc, resp, rad, slots_raw, slots, link, rows_of, select, place, weights, outgoing, sent, split, near_in, far_in, total,
    columns, keep, half_out, half_in, plane_out, plane_in, line_out, line_in,
    load_sem, resp_sem, face_send, face_recv, split_send, split_recv, half_send, half_recv, column_send, column_recv,
    plane_send, plane_recv, line_send, line_recv,
):
    loads = [
        pltpu.make_async_copy(face_index, slots_raw, load_sem.at[0]),
        pltpu.make_async_copy(incident, inc, load_sem.at[1]),
        pltpu.make_async_copy(linked, link, load_sem.at[2]),
    ]
    for load in loads:
        load.start()
    resp_loads = []
    for c in range(CHUNKS):
        rows = pl.ds(c * ROWS, ROWS)
        pair = [
            pltpu.make_async_copy(response.at[p, rows], resp.at[rows, pl.ds(p * M, M)], resp_sem.at[c, p])
            for p in range(2)
        ]
        resp_loads.append(pair)

    def start_response(c):
        for load in resp_loads[c]:
            load.start()

    start_response(0)
    rad_loads = [
        pltpu.make_async_copy(radiation.at[p], rad.at[:, pl.ds(p * M, M)], load_sem.at[3 + p]) for p in range(2)
    ]

    gx, gy, gz = lax.axis_index("gx"), lax.axis_index("gy"), lax.axis_index("gz")
    core, y_lo = gy % 2, gy // 2
    x, y_hi = gz % 4, gz // 4
    me_plane = gz * 2 + y_lo

    near_in[...] = jnp.zeros_like(near_in)
    for s in range(2):
        for g in range(3):
            far_in[s, g, 0:PAIR] = jnp.zeros((PAIR, EXC), BF16)
    plane_in[...] = jnp.zeros_like(plane_in)
    line_in[...] = jnp.zeros_like(line_in)

    barrier = pltpu.get_barrier_semaphore()

    def greet(device):
        pl.semaphore_signal(barrier, inc=1, device_id=device, device_id_type=MESH)

    def plane_peer(step):
        dyh, dx, dyl = step
        peer_gz = ((y_hi + dyh) % 2) * 4 + (x + dx) % 4
        peer_lo = (y_lo + dyl) % 2
        return peer_gz * 2 + peer_lo, (gx, peer_lo * 2 + core, peer_gz)

    order = plane_order()
    partner = (gx, gy + 1 - 2 * core, gz)
    cross = (gx, 3 - gy, gz)
    middle = (gy + 1) // 2 == 1
    for step in order:
        greet(plane_peer(step)[1])
    for d in range(1, 8):
        greet(((gx + d) % 8, gy, gz))
    greet(partner)
    greet(cross)
    for d in (1, 7):
        greet(((gx + d) % 8, gy + 1 - 2 * core, gz))
        greet((gx, gy + 1 - 2 * core, (gz + d) % 8))

    start_response(1)

    ahead, across = core, 1 - core
    face_of = (4 * ahead, 4 * ahead + 1, 4 * across, 4 * across + 1, 2 + core, 3 - core)
    place_a, place_b = gx * across + gz * ahead, gx * ahead + gz * across
    there = (place_a > 0, place_a < 7, place_b > 0, place_b < 7, middle, None)
    target = (
        (gx - across, gy, gz - ahead),
        (gx + across, gy, gz + ahead),
        (gx - ahead, gy, gz - across),
        (gx + ahead, gy, gz + across),
        cross,
        partner,
    )
    landing = (1, 0, 3, 2, 4, 5)

    def guarded(role, action):
        if there[role] is None:
            action()
        else:
            pl.when(there[role])(action)

    slots[...] = jnp.full(slots.shape, -1, jnp.int32)
    loads[0].wait()
    for f in range(6):
        slots[f : f + 1, 0:FACE] = slots_raw[f]
    lanes128 = lax.broadcasted_iota(jnp.int32, (128, 128), 1).astype(F32)
    for r in range(6):
        row = slots[pl.ds(face_of[r], 1), :].astype(F32)
        for half, count in ((0, 128), (1, 64)):
            wide = jnp.broadcast_to(row[:, half * 128 : (half + 1) * 128], (128, 128))
            tall = jnp.transpose(wide)[:count]
            for c in range(M // 128):
                hit = tall - float(c * 128) == lanes128[:count]
                start = (r % 2) * FACE + half * 128
                select[r // 2, start : start + count, c * 128 : (c + 1) * 128] = jnp.where(hit, 1.0, 0.0).astype(BF16)

    def set_weights(rows, real, imag):
        low = pl.ds(rows.start, rows.size)
        high = pl.ds(M + rows.start, rows.size)
        weights[low, 0:EXC] = real
        weights[low, EXC : 2 * EXC] = imag
        weights[high, 0:EXC] = -imag
        weights[high, EXC : 2 * EXC] = real

    start_response(2)
    loads[1].wait()
    for c in range(CHUNKS):
        rows = pl.ds(c * ROWS, ROWS)
        set_weights(rows, inc[0, rows], inc[1, rows])

    def respond(first):
        for c in range(CHUNKS):
            rows = pl.ds(c * ROWS, ROWS)
            if first:
                for load in resp_loads[c]:
                    load.wait()
                if c + 3 < CHUNKS:
                    start_response(c + 3)
                if c + 3 == CHUNKS:
                    for load in rad_loads:
                        load.start()
            outgoing[rows] = jnp.dot(resp[rows], weights[...], preferred_element_type=F32).astype(BF16)

    def face_copy(role, spot, device):
        return pltpu.make_async_remote_copy(
            src_ref=sent.at[role],
            dst_ref=near_in.at[pl.ds(spot * FACE, FACE)],
            send_sem=face_send.at[role],
            recv_sem=face_recv.at[spot],
            device_id=device,
            device_id_type=MESH,
        )

    def split_copy(role, half, into, g, up, device):
        return pltpu.make_async_remote_copy(
            src_ref=split.at[half, role],
            dst_ref=far_in.at[into, g, pl.ds(up * FACE, FACE)],
            send_sem=split_send.at[half, role],
            recv_sem=split_recv.at[into, 2 * g + up],
            device_id=device,
            device_id_type=MESH,
        )

    def halves(value, rows):
        odd = (lax.broadcasted_iota(jnp.int32, (rows, EXC), 1) // 4) % 2
        real, imag = value[:, 0:EXC], value[:, EXC : 2 * EXC]
        zero = jnp.where(odd == 0, real, pltpu.roll(imag, 4, 1))
        one = jnp.where(odd == 0, pltpu.roll(real, EXC - 4, 1), imag)
        return zero, one

    early = across * jnp.where((gz == 3) | (gz == 4), 1, 0)

    def send_faces(it):
        for g in (early, 1 - early, 2):
            picked = jnp.dot(select[g], outgoing[...], preferred_element_type=F32)
            if it == 0:
                rounded = picked.astype(BF16)
                for up in range(2):
                    sent[2 * g + up] = rounded[up * FACE : (up + 1) * FACE]
            else:
                for half, value in enumerate(halves(picked, PAIR)):
                    rounded = value.astype(BF16)
                    for up in range(2):
                        split[half, 2 * g + up] = rounded[up * FACE : (up + 1) * FACE]
            if isinstance(g, int):
                if it == 0:
                    pl.when(middle)(face_copy(4, 4, cross).start)
                    face_copy(5, 5, partner).start()
                else:
                    for half in range(2):
                        pl.when(middle)(split_copy(4, half, across, 2, 0, (gx, (1 - y_lo) * 2 + half, gz)).start)
                    split_copy(5, across, across, 2, 1, partner).start()
                    far_in[across, 2, FACE : 2 * FACE] = split[core, 5]
                continue
            along_x = (g + core) % 2
            along_z = 1 - along_x
            at = gx * along_z + gz * along_x
            for up in range(2):
                move = 2 * up - 1
                inside = at != 7 * up
                if it == 0:
                    device = (gx + along_z * move, gy, gz + along_x * move)
                    pl.when(inside)(face_copy(2 * g + up, 2 * g + 1 - up, device).start)
                    continue
                for half in range(2):
                    device = (gx + along_z * move, y_lo * 2 + half, gz + along_x * move)
                    pl.when(inside)(split_copy(2 * g + up, half, core, g, 1 - up, device).start)

    def take_faces(roles):
        for r in roles:
            guarded(r, face_copy(r, r, target[r]).wait_recv)

    def take_halves(g):
        for s in range(2):
            for up in range(2):
                wait = split_copy(2 * g + up, 0, s, g, up, partner).wait_recv
                if g == 2:
                    pl.when(s == core if up else s != y_lo)(wait)
                else:
                    spot = gx if (g + s) % 2 == 0 else gz
                    pl.when(spot < 7 if up else spot > 0)(wait)

    def add_traces():
        for n, g in enumerate(TAKE_ORDER):
            take_faces((2 * g, 2 * g + 1))
            span = slice(g * PAIR, (g + 1) * PAIR)
            for c in range(CHUNKS):
                rows = pl.ds(c * ROWS, ROWS)
                trace = jnp.dot(place[rows, span], near_in[span], preferred_element_type=F32)
                if n > 0:
                    trace = trace + total[rows]
                if n < 2:
                    total[rows] = trace
                else:
                    real = (trace[:, 0:EXC] + inc[0, rows].astype(F32)).astype(BF16)
                    imag = (trace[:, EXC : 2 * EXC] + inc[1, rows].astype(F32)).astype(BF16)
                    set_weights(rows, real, imag)

    def column_copy(s, g):
        return pltpu.make_async_remote_copy(
            src_ref=columns.at[s, g],
            dst_ref=columns.at[s, g],
            send_sem=column_send.at[g],
            recv_sem=column_recv.at[g],
            device_id=partner,
            device_id_type=MESH,
        )

    def gather_columns(g):
        for p in range(2):
            picked = jnp.dot(
                rad[:, p * M : (p + 1) * M], place[:, g * PAIR : (g + 1) * PAIR], preferred_element_type=F32
            )
            columns[core, g, :, p * PAIR : (p + 1) * PAIR] = picked.astype(BF16)
        column_copy(core, g).start()

    respond(True)
    pl.semaphore_wait(barrier, 15 + 7 + 2 + 4)
    send_faces(0)

    for load in rad_loads:
        load.wait()
    half_copies = []
    for q in range(PARTS):
        rows = pl.ds(q * PART_ROWS, PART_ROWS)
        zero, one = halves(jnp.dot(rad[rows], weights[...], preferred_element_type=F32), PART_ROWS)
        keep[rows] = jnp.where(core == 0, zero, one)
        half_out[rows] = jnp.where(core == 0, one, zero)
        half_copies.append(
            pltpu.make_async_remote_copy(
                src_ref=half_out.at[rows],
                dst_ref=half_in.at[rows],
                send_sem=half_send.at[q],
                recv_sem=half_recv.at[q],
                device_id=partner,
                device_id_type=MESH,
            )
        )
        half_copies[q].start()
    loads[2].wait()
    for r in range(6):
        row = jnp.where(link[0, face_of[r]] > 0, slots_raw[face_of[r]], -1)
        rows_of[r // 2 : r // 2 + 1, (r % 2) * FACE : (r % 2 + 1) * FACE] = row
    for g in range(3):
        row = rows_of[g : g + 1, :]
        for c in range(CHUNKS):
            spots = lax.broadcasted_iota(jnp.int32, (ROWS, PAIR), 0) + c * ROWS
            place[c * ROWS : (c + 1) * ROWS, g * PAIR : (g + 1) * PAIR] = jnp.where(spots == row, 1.0, 0.0).astype(BF16)
    gather_columns(TAKE_ORDER[0])

    add_traces()
    respond(False)
    send_faces(1)
    for g in TAKE_ORDER[1:]:
        gather_columns(g)

    odd_part = (lax.broadcasted_iota(jnp.int32, (PAIR, EXC), 1) // 4) % 2
    small = lax.broadcasted_iota(jnp.int32, (BLOCK // 2, EXC), 1)
    odd_lo = (small // 8) % 2
    plane_copies = []
    for copy in half_copies:
        copy.wait_recv()
    for n, g in enumerate(TAKE_ORDER):
        column_copy(across, g).wait_recv()
        take_halves(g)
        for s in range(2):
            faces = far_in[s, g, 0:PAIR].astype(F32)
            turned = jnp.where(odd_part == 0, -pltpu.roll(faces, EXC - 4, 1), pltpu.roll(faces, 4, 1))
            far_in[s, g, PAIR : 2 * PAIR] = turned.astype(BF16)
        for q in range(PARTS):
            part = q if n < 2 else (1 - y_hi if q == 0 else y_hi)
            rows = pl.ds(pl.multiple_of(part * PART_ROWS, PART_ROWS), PART_ROWS)
            value = keep[rows]
            if n == 0:
                value = value + half_in[rows]
            for s in range(2):
                value = value + jnp.dot(columns[s, g, rows], far_in[s, g], preferred_element_type=F32)
            if n < 2:
                keep[rows] = value
                continue
            for b in range(PART_ROWS // BLOCK):
                top = value[b * BLOCK : b * BLOCK + BLOCK // 2]
                low = value[b * BLOCK + BLOCK // 2 : (b + 1) * BLOCK]
                slot = (part * (PART_ROWS // BLOCK) + b) * 2
                plane_out[slot] = jnp.where(odd_lo == 0, top, pltpu.roll(low, 8, 1)).astype(BF16)
                plane_out[slot + 1] = jnp.where(odd_lo == 0, pltpu.roll(top, EXC - 8, 1), low).astype(BF16)
            for k, step in enumerate(order):
                if step[0] == q:
                    continue
                peer, device = plane_peer(step)
                copy = pltpu.make_async_remote_copy(
                    src_ref=plane_out.at[peer],
                    dst_ref=plane_in.at[me_plane],
                    send_sem=plane_send.at[k],
                    recv_sem=plane_recv.at[me_plane],
                    device_id=device,
                    device_id_type=MESH,
                )
                copy.start()
                plane_copies.append(copy)

    for s in range(16):

        @pl.when(s != me_plane)
        def _():
            pltpu.make_async_remote_copy(
                src_ref=plane_out.at[s],
                dst_ref=plane_in.at[s],
                send_sem=plane_send.at[0],
                recv_sem=plane_recv.at[s],
                device_id=partner,
                device_id_type=MESH,
            ).wait_recv()

    piece = plane_out[me_plane].astype(F32)
    for s in range(16):
        piece = piece + plane_in[s].astype(F32)
    tall = jnp.concatenate([piece, pltpu.roll(piece, EXC - 8, 1)], axis=0)
    turned = jnp.transpose(jnp.concatenate([tall, tall], axis=0))
    for d in range(8):
        line_out[d] = turned[d * 16 : d * 16 + 8]
    line_copies = []
    for d in (4, 3, 5, 2, 6, 1, 7):
        peer = (gx + d) % 8
        copy = pltpu.make_async_remote_copy(
            src_ref=line_out.at[peer],
            dst_ref=line_in.at[gx],
            send_sem=line_send.at[d],
            recv_sem=line_recv.at[gx],
            device_id=(peer, gy, gz),
            device_id_type=MESH,
        )
        copy.start()
        line_copies.append(copy)

    for r in range(6):
        guarded(r, face_copy(r, landing[r], target[r]).wait_send)
        for half in range(2):
            if r < 5:
                guarded(r, split_copy(r, half, 0, 0, 0, target[r]).wait_send)
    split_copy(5, across, 0, 0, 0, partner).wait_send()
    for g in range(3):
        column_copy(core, g).wait_send()
    for copy in half_copies + plane_copies:
        copy.wait_send()

    for s in range(8):

        @pl.when(s != gx)
        def _():
            pltpu.make_async_remote_copy(
                src_ref=line_out.at[s],
                dst_ref=line_in.at[s],
                send_sem=line_send.at[0],
                recv_sem=line_recv.at[s],
                device_id=partner,
                device_id_type=MESH,
            ).wait_recv()

    result = line_out[gx]
    for s in range(8):
        result = result + line_in[s]
    out_ref[0] = result[0:4, 0:BLOCK]
    out_ref[1] = result[4:8, 0:BLOCK]
    for copy in line_copies:
        copy.wait_send()


def shards(incident, response, radiation, face_index, linked):
    anywhere = pl.BlockSpec(memory_space=pl.ANY)
    dma = pltpu.SemaphoreType.DMA
    return pl.pallas_call(
        kernel,
        out_shape=pltpu.VMEM((2, 4, BLOCK), F32),
        in_specs=[anywhere] * 5,
        out_specs=pl.BlockSpec(memory_space=pltpu.VMEM),
        scratch_shapes=[
            pltpu.VMEM((2, M, EXC), BF16),
            pltpu.VMEM((M, 2 * M), BF16),
            pltpu.VMEM((ANG, 2 * M), BF16),
            pltpu.VMEM((6, 1, FACE), jnp.int32),
            pltpu.VMEM((8, PADDED), jnp.int32),
            pltpu.SMEM((1, 6), jnp.int32),
            pltpu.VMEM((8, PAIR), jnp.int32),
            pltpu.VMEM((3, PAIR, M), BF16),
            pltpu.VMEM((M, 3 * PAIR), BF16),
            pltpu.VMEM((2 * M, 2 * EXC), BF16),
            pltpu.VMEM((M, 2 * EXC), BF16),
            pltpu.VMEM((6, FACE, 2 * EXC), BF16),
            pltpu.VMEM((2, 6, FACE, EXC), BF16),
            pltpu.VMEM((3 * PAIR, 2 * EXC), BF16),
            pltpu.VMEM((2, 3, 2 * PAIR, EXC), BF16),
            pltpu.VMEM((M, 2 * EXC), F32),
            pltpu.VMEM((2, 3, ANG, 2 * PAIR), BF16),
            pltpu.VMEM((ANG, EXC), F32),
            pltpu.VMEM((ANG, EXC), F32),
            pltpu.VMEM((ANG, EXC), F32),
            pltpu.VMEM((16, BLOCK // 2, EXC), BF16),
            pltpu.VMEM((16, BLOCK // 2, EXC), BF16),
            pltpu.VMEM((8, 8, EXC), F32),
            pltpu.VMEM((8, 8, EXC), F32),
            dma((5,)),
            dma((CHUNKS, 2)),
            dma((6,)),
            dma((6,)),
            dma((2, 6)),
            dma((2, 6)),
            dma((PARTS,)),
            dma((PARTS,)),
            dma((3,)),
            dma((3,)),
            dma((16,)),
            dma((16,)),
            dma((8,)),
            dma((8,)),
        ],
        compiler_params=pltpu.CompilerParams(
            collective_id=0, has_side_effects=True, vmem_limit_bytes=60 * 1024 * 1024
        ),
        cost_estimate=pl.CostEstimate(flops=8_000_000_000, bytes_accessed=10_000_000, transcendentals=0),
        name="schwarz",
    )(
        incident.reshape(2, M, EXC),
        response.reshape(2, M, M),
        radiation.reshape(2, ANG, M),
        face_index.reshape(6, 1, FACE),
        linked.reshape(1, 6),
    )


def solution(mesh):
    return jax.shard_map(
        shards,
        mesh=mesh,
        in_specs=(
            P("gx", "gy", "gz", None, None, None),
            P("gx", "gy", "gz", None, None, None),
            P("gx", "gy", "gz", None, None, None),
            P("gx", "gy", "gz", None, None),
            P("gx", "gy", "gz", None),
        ),
        out_specs=P(None, ("gx", "gy"), "gz"),
        check_vma=False,
    )
```

```python
import functools

import jax
import jax.numpy as jnp
from jax import lax
from jax.experimental import pallas as pl
from jax.experimental.pallas import tpu as pltpu
from jax.sharding import PartitionSpec as P

M = 1280
FACE = 192
ANG = 512
EXC = 128
PADDED = 256
CHUNKS = 5
ROWS = M // CHUNKS
PARTS = 4
PART_ROWS = ANG // PARTS
BLOCK = 64
MESH = pl.DeviceIdType.MESH
TAKE_ORDER = (0, 2, 1)
BF16, F32 = jnp.bfloat16, jnp.float32


def plane_order():
    steps = [(a, b, c) for a in range(2) for b in range(4) for c in range(2) if (a, b, c) != (0, 0, 0)]
    return sorted(steps, key=lambda s: -((2 if s[1] == 2 else s[1] % 2) + (1 if s[2] else 2 * s[0])))


def kernel(
    incident, response, radiation, face_index, linked, out_ref,
    inc, resp, rad, slots_raw, slots, link, select, place, weights, outgoing, sent, near_in, far_in, total, columns, field,
    keep, half_out, half_in, plane_out, plane_in, line_out, line_in,
    load_sem, resp_sem, face_send, face_recv, half_send, half_recv, plane_send, plane_recv, line_send, line_recv,
):
    loads = [
        pltpu.make_async_copy(face_index, slots_raw, load_sem.at[0]),
        pltpu.make_async_copy(incident, inc, load_sem.at[1]),
        pltpu.make_async_copy(linked, link, load_sem.at[2]),
    ]
    for load in loads:
        load.start()
    resp_loads = []
    for c in range(CHUNKS):
        rows = pl.ds(c * ROWS, ROWS)
        pair = [
            pltpu.make_async_copy(response.at[p, rows], resp.at[rows, pl.ds(p * M, M)], resp_sem.at[c, p])
            for p in range(2)
        ]
        resp_loads.append(pair)

    def start_response(c):
        for load in resp_loads[c]:
            load.start()

    start_response(0)
    rad_loads = [
        pltpu.make_async_copy(radiation.at[p], rad.at[:, pl.ds(p * M, M)], load_sem.at[3 + p]) for p in range(2)
    ]

    gx, gy, gz = lax.axis_index("gx"), lax.axis_index("gy"), lax.axis_index("gz")
    core, y_lo = gy % 2, gy // 2
    x, y_hi = gz % 4, gz // 4
    me_plane = gz * 2 + y_lo

    near_in[...] = jnp.zeros_like(near_in)
    for g in range(3):
        far_in[g, 0 : 2 * PADDED] = jnp.zeros((2 * PADDED, 2 * EXC), BF16)
    plane_in[...] = jnp.zeros_like(plane_in)
    line_in[...] = jnp.zeros_like(line_in)

    barrier = pltpu.get_barrier_semaphore()

    def greet(device):
        pl.semaphore_signal(barrier, inc=1, device_id=device, device_id_type=MESH)

    def plane_peer(step):
        dyh, dx, dyl = step
        peer_gz = ((y_hi + dyh) % 2) * 4 + (x + dx) % 4
        peer_lo = (y_lo + dyl) % 2
        return peer_gz * 2 + peer_lo, (gx, peer_lo * 2 + core, peer_gz)

    order = plane_order()
    partner = (gx, gy + 1 - 2 * core, gz)
    cross = (gx, 3 - gy, gz)
    middle = (gy + 1) // 2 == 1
    for step in order:
        greet(plane_peer(step)[1])
    for d in range(1, 8):
        greet(((gx + d) % 8, gy, gz))
    greet(partner)

    @pl.when(middle)
    def _():
        greet(cross)

    start_response(1)

    ahead, across = core, 1 - core
    face_of = (4 * ahead, 4 * ahead + 1, 4 * across, 4 * across + 1, 2 + core, 3 - core)
    place_a, place_b = gx * across + gz * ahead, gx * ahead + gz * across
    there = (place_a > 0, place_a < 7, place_b > 0, place_b < 7, middle, None)
    target = (
        (gx - across, gy, gz - ahead),
        (gx + across, gy, gz + ahead),
        (gx - ahead, gy, gz - across),
        (gx + ahead, gy, gz + across),
        cross,
        partner,
    )
    landing = (1, 0, 3, 2, 4, 5)

    def guarded(role, action):
        if there[role] is None:
            action()
        else:
            pl.when(there[role])(action)

    slots[...] = jnp.full(slots.shape, -1, jnp.int32)
    loads[0].wait()
    for f in range(6):
        slots[f : f + 1, 0:FACE] = slots_raw[f]
    lanes128 = lax.broadcasted_iota(jnp.int32, (128, 128), 1).astype(F32)
    for r in range(6):
        row = slots[pl.ds(face_of[r], 1), :].astype(F32)
        for half, count in ((0, 128), (1, 64)):
            wide = jnp.broadcast_to(row[:, half * 128 : (half + 1) * 128], (128, 128))
            tall = jnp.transpose(wide)[:count]
            for c in range(M // 128):
                hit = tall - float(c * 128) == lanes128[:count]
                start = (r % 2) * FACE + half * 128
                select[r // 2, start : start + count, c * 128 : (c + 1) * 128] = jnp.where(hit, 1.0, 0.0).astype(BF16)

    def set_weights(rows, real, imag):
        low = pl.ds(rows.start, rows.size)
        high = pl.ds(M + rows.start, rows.size)
        weights[low, 0:EXC] = real
        weights[low, EXC : 2 * EXC] = imag
        weights[high, 0:EXC] = -imag
        weights[high, EXC : 2 * EXC] = real

    start_response(2)
    loads[1].wait()
    for c in range(CHUNKS):
        rows = pl.ds(c * ROWS, ROWS)
        set_weights(rows, inc[0, rows], inc[1, rows])

    def respond(first):
        for c in range(CHUNKS):
            rows = pl.ds(c * ROWS, ROWS)
            if first:
                for load in resp_loads[c]:
                    load.wait()
                if c + 3 < CHUNKS:
                    start_response(c + 3)
                if c + 3 == CHUNKS:
                    for load in rad_loads:
                        load.start()
            outgoing[rows] = jnp.dot(resp[rows], weights[...], preferred_element_type=F32).astype(BF16)

    def into(it, spot):
        if it == 0:
            return near_in.at[pl.ds(spot * PADDED, FACE)]
        return far_in.at[spot // 2, pl.ds((spot % 2) * PADDED, FACE)]

    def face_copy(it, role, spot, device):
        return pltpu.make_async_remote_copy(
            src_ref=sent.at[it, role],
            dst_ref=into(it, spot),
            send_sem=face_send.at[it, role],
            recv_sem=face_recv.at[it, spot],
            device_id=device,
            device_id_type=MESH,
        )

    early = across * jnp.where((gz == 3) | (gz == 4), 1, 0)

    def send_faces(it):
        for g in (early, 1 - early, 2):
            picked = jnp.dot(select[g], outgoing[...], preferred_element_type=F32).astype(BF16)
            for up in range(2):
                sent[it, 2 * g + up] = picked[up * FACE : (up + 1) * FACE]
            if isinstance(g, int):
                pl.when(middle)(face_copy(it, 4, 4, cross).start)
                face_copy(it, 5, 5, partner).start()
                continue
            along_x = (g + core) % 2
            along_z = 1 - along_x
            at = gx * along_z + gz * along_x
            for up in range(2):
                move = 2 * up - 1
                device = (gx + along_z * move, gy, gz + along_x * move)
                pl.when(at != 7 * up)(face_copy(it, 2 * g + up, 2 * g + 1 - up, device).start)

    def take_faces(it, roles):
        for r in roles:
            guarded(r, face_copy(it, r, r, target[r]).wait_recv)

    def add_traces():
        for n, g in enumerate(TAKE_ORDER):
            take_faces(0, (2 * g, 2 * g + 1))
            span = slice(2 * g * PADDED, (2 * g + 2) * PADDED)
            for c in range(CHUNKS):
                rows = pl.ds(c * ROWS, ROWS)
                trace = jnp.dot(place[rows, span], near_in[span], preferred_element_type=F32)
                if n > 0:
                    trace = trace + total[rows]
                if n < 2:
                    total[rows] = trace
                else:
                    real = (trace[:, 0:EXC] + inc[0, rows].astype(F32)).astype(BF16)
                    imag = (trace[:, EXC : 2 * EXC] + inc[1, rows].astype(F32)).astype(BF16)
                    set_weights(rows, real, imag)

    def gather_columns(g, p):
        picked = jnp.dot(
            rad[:, p * M : (p + 1) * M], place[:, 2 * g * PADDED : (2 * g + 2) * PADDED], preferred_element_type=F32
        )
        columns[g, :, 2 * p * PADDED : (2 * p + 2) * PADDED] = picked.astype(BF16)

    respond(True)
    pl.semaphore_wait(barrier, 15 + 7 + 1 + jnp.where(middle, 1, 0))
    send_faces(0)

    for load in rad_loads:
        load.wait()
    field[...] = jnp.dot(rad[...], weights[...], preferred_element_type=F32)
    loads[2].wait()
    for r in range(6):
        row = jnp.where(link[0, face_of[r]] > 0, slots[pl.ds(face_of[r], 1), :], -1)
        for c in range(CHUNKS):
            spots = lax.broadcasted_iota(jnp.int32, (ROWS, PADDED), 0) + c * ROWS
            place[c * ROWS : (c + 1) * ROWS, r * PADDED : (r + 1) * PADDED] = jnp.where(spots == row, 1.0, 0.0).astype(BF16)
    gather_columns(TAKE_ORDER[0], 0)
    gather_columns(TAKE_ORDER[0], 1)

    add_traces()
    respond(False)
    send_faces(1)
    for g in TAKE_ORDER[1:]:
        gather_columns(g, 0)
        gather_columns(g, 1)

    lanes = lax.broadcasted_iota(jnp.int32, (PART_ROWS, EXC), 1)
    odd_core = (lanes // 4) % 2
    half_copies = []
    parts = [(1 - y_hi) * 2, (1 - y_hi) * 2 + 1, y_hi * 2, y_hi * 2 + 1]
    for n, g in enumerate(TAKE_ORDER):
        take_faces(1, (2 * g, 2 * g + 1))
        low, high = slice(0, 2 * PADDED), slice(2 * PADDED, 4 * PADDED)
        far_in[g, high, 0:EXC] = -far_in[g, low, EXC : 2 * EXC]
        far_in[g, high, EXC : 2 * EXC] = far_in[g, low, 0:EXC]
        for q in range(PARTS):
            part = q if n < 2 else parts[q]
            rows = pl.ds(pl.multiple_of(part * PART_ROWS, PART_ROWS), PART_ROWS)
            value = field[rows] + jnp.dot(columns[g, rows], far_in[g], preferred_element_type=F32)
            if n < 2:
                field[rows] = value
                continue
            real, imag = value[:, 0:EXC], value[:, EXC : 2 * EXC]
            zero = jnp.where(odd_core == 0, real, pltpu.roll(imag, 4, 1))
            one = jnp.where(odd_core == 0, pltpu.roll(real, EXC - 4, 1), imag)
            keep[rows] = jnp.where(core == 0, zero, one)
            half_out[rows] = jnp.where(core == 0, one, zero)
            copy = pltpu.make_async_remote_copy(
                src_ref=half_out.at[rows],
                dst_ref=half_in.at[rows],
                send_sem=half_send.at[q],
                recv_sem=half_recv.at[q],
                device_id=partner,
                device_id_type=MESH,
            )
            copy.start()
            half_copies.append(copy)

    small = lax.broadcasted_iota(jnp.int32, (BLOCK // 2, EXC), 1)
    odd_lo = (small // 8) % 2
    plane_copies = []
    for q in range(PARTS):
        half_copies[q].wait_recv()
        for b in range(PART_ROWS // BLOCK):
            start = parts[q] * PART_ROWS + b * BLOCK
            first = pl.ds(pl.multiple_of(start, BLOCK // 2), BLOCK // 2)
            second = pl.ds(pl.multiple_of(start + BLOCK // 2, BLOCK // 2), BLOCK // 2)
            top = keep[first] + half_in[first]
            low = keep[second] + half_in[second]
            slot = (parts[q] * (PART_ROWS // BLOCK) + b) * 2
            plane_out[slot] = jnp.where(odd_lo == 0, top, pltpu.roll(low, 8, 1)).astype(BF16)
            plane_out[slot + 1] = jnp.where(odd_lo == 0, pltpu.roll(top, EXC - 8, 1), low).astype(BF16)
        if q % 2 == 0:
            continue
        for k, step in enumerate(order):
            if step[0] == q // 2:
                continue
            peer, device = plane_peer(step)
            copy = pltpu.make_async_remote_copy(
                src_ref=plane_out.at[peer],
                dst_ref=plane_in.at[me_plane],
                send_sem=plane_send.at[k],
                recv_sem=plane_recv.at[me_plane],
                device_id=device,
                device_id_type=MESH,
            )
            copy.start()
            plane_copies.append(copy)

    for s in range(16):

        @pl.when(s != me_plane)
        def _():
            pltpu.make_async_remote_copy(
                src_ref=plane_out.at[s],
                dst_ref=plane_in.at[s],
                send_sem=plane_send.at[0],
                recv_sem=plane_recv.at[s],
                device_id=partner,
                device_id_type=MESH,
            ).wait_recv()

    piece = plane_out[me_plane].astype(F32)
    for s in range(16):
        piece = piece + plane_in[s].astype(F32)
    tall = jnp.concatenate([piece, pltpu.roll(piece, EXC - 8, 1)], axis=0)
    turned = jnp.transpose(jnp.concatenate([tall, tall], axis=0))
    for d in range(8):
        line_out[d] = turned[d * 16 : d * 16 + 8]
    line_copies = []
    for d in (4, 3, 5, 2, 6, 1, 7):
        peer = (gx + d) % 8
        copy = pltpu.make_async_remote_copy(
            src_ref=line_out.at[peer],
            dst_ref=line_in.at[gx],
            send_sem=line_send.at[d],
            recv_sem=line_recv.at[gx],
            device_id=(peer, gy, gz),
            device_id_type=MESH,
        )
        copy.start()
        line_copies.append(copy)

    for it in range(2):
        for r in range(6):
            guarded(r, face_copy(it, r, landing[r], target[r]).wait_send)
    for copy in half_copies + plane_copies:
        copy.wait_send()

    for s in range(8):

        @pl.when(s != gx)
        def _():
            pltpu.make_async_remote_copy(
                src_ref=line_out.at[s],
                dst_ref=line_in.at[s],
                send_sem=line_send.at[0],
                recv_sem=line_recv.at[s],
                device_id=partner,
                device_id_type=MESH,
            ).wait_recv()

    result = line_out[gx]
    for s in range(8):
        result = result + line_in[s]
    out_ref[0] = result[0:4, 0:BLOCK]
    out_ref[1] = result[4:8, 0:BLOCK]
    for copy in line_copies:
        copy.wait_send()


def shards(incident, response, radiation, face_index, linked):
    anywhere = pl.BlockSpec(memory_space=pl.ANY)
    dma = pltpu.SemaphoreType.DMA
    return pl.pallas_call(
        kernel,
        out_shape=pltpu.VMEM((2, 4, BLOCK), F32),
        in_specs=[anywhere] * 5,
        out_specs=pl.BlockSpec(memory_space=pltpu.VMEM),
        scratch_shapes=[
            pltpu.VMEM((2, M, EXC), BF16),
            pltpu.VMEM((M, 2 * M), BF16),
            pltpu.VMEM((ANG, 2 * M), BF16),
            pltpu.VMEM((6, 1, FACE), jnp.int32),
            pltpu.VMEM((8, PADDED), jnp.int32),
            pltpu.SMEM((1, 6), jnp.int32),
            pltpu.VMEM((3, 2 * FACE, M), BF16),
            pltpu.VMEM((M, 6 * PADDED), BF16),
            pltpu.VMEM((2 * M, 2 * EXC), BF16),
            pltpu.VMEM((M, 2 * EXC), BF16),
            pltpu.VMEM((2, 6, FACE, 2 * EXC), BF16),
            pltpu.VMEM((6 * PADDED, 2 * EXC), BF16),
            pltpu.VMEM((3, 4 * PADDED, 2 * EXC), BF16),
            pltpu.VMEM((M, 2 * EXC), F32),
            pltpu.VMEM((3, ANG, 4 * PADDED), BF16),
            pltpu.VMEM((ANG, 2 * EXC), F32),
            pltpu.VMEM((ANG, EXC), F32),
            pltpu.VMEM((ANG, EXC), F32),
            pltpu.VMEM((ANG, EXC), F32),
            pltpu.VMEM((16, BLOCK // 2, EXC), BF16),
            pltpu.VMEM((16, BLOCK // 2, EXC), BF16),
            pltpu.VMEM((8, 8, EXC), F32),
            pltpu.VMEM((8, 8, EXC), F32),
            dma((5,)),
            dma((CHUNKS, 2)),
            dma((2, 6)),
            dma((2, 6)),
            dma((PARTS,)),
            dma((PARTS,)),
            dma((16,)),
            dma((16,)),
            dma((8,)),
            dma((8,)),
        ],
        compiler_params=pltpu.CompilerParams(
            collective_id=0, has_side_effects=True, vmem_limit_bytes=60 * 1024 * 1024
        ),
        cost_estimate=pl.CostEstimate(flops=8_000_000_000, bytes_accessed=10_000_000, transcendentals=0),
        name="schwarz",
    )(
        incident.reshape(2, M, EXC),
        response.reshape(2, M, M),
        radiation.reshape(2, ANG, M),
        face_index.reshape(6, 1, FACE),
        linked.reshape(1, 6),
    )


def solution(mesh):
    return jax.shard_map(
        shards,
        mesh=mesh,
        in_specs=(
            P("gx", "gy", "gz", None, None, None),
            P("gx", "gy", "gz", None, None, None),
            P("gx", "gy", "gz", None, None, None),
            P("gx", "gy", "gz", None, None),
            P("gx", "gy", "gz", None),
        ),
        out_specs=P(None, ("gx", "gy"), "gz"),
        check_vma=False,
    )
```
